32 devices in a mesh: cluster: 8 (over z, y), sub: 4 (over x, core).
Axes of the slice: x: 2, y: 2, z: 4, core: 2. Of those that a mesh axis runs over, the one named last changes fastest.
Arguments:
- rhs: float32 [128, 4, 384], P(('cluster', 'sub')), may hold values from -8 to 8
- operators: bfloat16 [128, 384, 384], P(('cluster', 'sub')), may hold values from -1 to 5
- signs: int32 [128, 384], P(('cluster', 'sub')), may hold values from -1 to 1, as said below
- links: int32 [128, 3, 128], P(('cluster', 'sub')), may hold values from 0 to 127, as said below
- cluster_basis: float32 [128, 24, 384], P(('cluster', 'sub')), may hold values from -0.3125 to 0.3125
- corner_basis: float32 [128, 8, 384], P(('cluster', 'sub')), may hold values from -0.3125 to 0.3125
- corner_ids: int32 [128, 8], P(('cluster', 'sub')), may hold values from 0 to 127
- cluster_coarse: float32 [8, 384, 384], P('cluster', 'sub'), may hold values from -1 to 3
- global_coarse: float32 [128, 128], P('sub'), may hold values from -0.2 to 0.5
Outputs:
- multipliers: float32 [128, 4, 384], P(('cluster', 'sub'))
- residual: float32 [128, 4, 384], P(('cluster', 'sub'))
The draws below stay inside these ranges and needn't reach their ends.
Inputs may be any that keep to these rules, and one draw needn't show every extreme that they name: `signs`: each entry is -1 or 1. Each links[s, b] is a permutation of 0 to 127; both subdomains of an interface pair hold the same permutation for it.
All inputs are finite; a program needn't handle non-finite values.
Results may differ from the reference program's by a relative error of at most 0.007.
Values sent between devices are 32-bit elements; how exact they have to be, the bound alone decides.
A program may use at most 64 MiB of HBM per device.

```python
import math
from functools import partial
import jax
import jax.numpy as jnp
from jax import lax

SUB_DEV = 4
LOADS = 4
BLK = 128
KC = 24
CORN = 8
ITERS = 2
DUAL = 384
CLUSTERS = 8
SUBS = 128
CCO = 384
NG = 128
N_SUB = 4


def draw_rhs(key, part):
    position = jnp.arange(SUBS, dtype=jnp.float32) / SUBS
    values = jnp.clip(jax.random.normal(key, (SUBS, LOADS, DUAL), jnp.float32), -4.0, 4.0)
    scaling = 0.6 + 1.2 * position
    return values * scaling[:, None, None]


def draw_operators(key, part):
    first_key, second_key = jax.random.split(key)
    identity = jnp.eye(DUAL, dtype=jnp.float32)
    diagonal = jnp.exp(jax.random.uniform(first_key, (SUBS, DUAL), jnp.float32, 0.0, math.log(4.0)))
    coupling = jnp.clip(jax.random.normal(second_key, (SUBS, DUAL, DUAL), jnp.float32), -4.0, 4.0) * (0.3 / math.sqrt(DUAL))
    return (coupling * (1.0 - identity) + diagonal[:, :, None] * identity).astype(jnp.bfloat16)


def coarse_matrix(key, leading, order):
    second_key = jax.random.fold_in(key, 1)
    identity = jnp.eye(order, dtype=jnp.float32)
    diagonal = jnp.ones(leading + (order,), jnp.float32)
    coupling = jnp.clip(jax.random.normal(second_key, leading + (order, order), jnp.float32), -4.0, 4.0) * (0.5 / math.sqrt(order))
    return coupling * (1.0 - identity) + diagonal[..., None] * identity


def draw_cluster_coarse(key, part):
    return coarse_matrix(key, (CLUSTERS,), CCO)


def draw_global_coarse(key, part):
    return 0.15 * coarse_matrix(key, (), NG)


def draw_signs(key, part):
    return 2 * jax.random.randint(key, (SUBS, DUAL), 0, 2, jnp.int32) - 1


def shuffle(base_key, pair_id):
    return jax.random.permutation(jax.random.fold_in(base_key, pair_id), BLK)


def draw_links(key, part):
    numbers = jnp.arange(SUBS, dtype=jnp.int32)
    member = numbers % SUB_DEV
    position = numbers // SUB_DEV % N_SUB
    cluster = numbers // (SUB_DEV * N_SUB)
    stride = SUB_DEV * N_SUB
    down_pair = jnp.where(position > 0, numbers - SUB_DEV, numbers + SUBS)
    across_pair = jnp.where(member % 2 == 0, numbers, jnp.where(cluster > 0, numbers - stride - 1, numbers + SUBS))
    inside_key = jax.random.fold_in(key, 11)
    outside_key = jax.random.fold_in(key, 23)
    up_order = jax.vmap(partial(shuffle, inside_key))(numbers)
    down_order = jax.vmap(partial(shuffle, inside_key))(down_pair)
    across_order = jax.vmap(partial(shuffle, outside_key))(across_pair)
    return jnp.stack([up_order, down_order, across_order], axis=1).astype(jnp.int32)


def with_ends(values, stream_key, least, largest):
    index_at = [jax.random.randint(jax.random.fold_in(stream_key, axis), (), 0, length) for axis, length in enumerate(values.shape)]
    widest = values.shape.index(max(values.shape))
    neighbour = index_at[:widest] + [(index_at[widest] + 1) % values.shape[widest]] + index_at[widest + 1:]
    return values.at[tuple(index_at)].set(least).at[tuple(neighbour)].set(largest)


def shard_levels(stream_key, shape, pieces, smallest, largest):
    factor_of = 1.0
    for dim, blocks in pieces:
        draws = jax.random.uniform(jax.random.fold_in(jax.random.fold_in(stream_key, 6), dim), (blocks,), jnp.float32, smallest / len(pieces), largest / len(pieces))
        factor_of = factor_of * jnp.repeat(jnp.exp(draws), shape[dim] // blocks).reshape((-1,) + (1,) * (len(shape) - 1 - dim))
    return factor_of


def scatter_about(key, shape, deviation, most, pieces=(), held_as=jnp.bfloat16):
    entries = jax.random.normal(key, shape, jnp.float32) * deviation
    if len(pieces) > 0:
        entries = shard_levels(key, shape, pieces, -0.22, 0.18) * entries
    return jnp.clip(entries, min=-most, max=most).astype(held_as)


def setup_inputs(seed: int = 0) -> dict:
    streams_of = jax.random.split(jax.random.key(seed), 10)
    rhs = draw_rhs(jax.random.fold_in(streams_of[9], 71), 0)
    operators = draw_operators(jax.random.fold_in(streams_of[9], 71), 0)
    signs = draw_signs(jax.random.fold_in(streams_of[9], 71), 0)
    links = draw_links(jax.random.fold_in(streams_of[9], 71), 0)
    cluster_basis = scatter_about(streams_of[4], (SUBS, KC, DUAL), DUAL ** -0.5, 0.3125, ((0, 32),), jnp.float32)
    corner_basis = scatter_about(streams_of[5], (SUBS, CORN, DUAL), DUAL ** -0.5, 0.3125, ((0, 32),), jnp.float32)
    corner_ids = with_ends(jax.random.randint(streams_of[6], (SUBS, CORN), 0, NG), jax.random.fold_in(streams_of[6], 1), 0, NG - 1).astype(jnp.int32)
    cluster_coarse = draw_cluster_coarse(jax.random.fold_in(streams_of[9], 71), 0)
    global_coarse = draw_global_coarse(jax.random.fold_in(streams_of[9], 71), 0)
    return {"rhs": rhs, "operators": operators, "signs": signs, "links": links, "cluster_basis": cluster_basis, "corner_basis": corner_basis, "corner_ids": corner_ids, "cluster_coarse": cluster_coarse, "global_coarse": global_coarse}


HIGHEST_PRECISION = lax.Precision.HIGHEST


def invert(order):
    row_index = jnp.broadcast_to(jnp.arange(order.shape[0], dtype=jnp.int32)[:, None], order.shape)
    col_index = jnp.broadcast_to(jnp.arange(order.shape[1], dtype=jnp.int32)[None, :], order.shape)
    return jnp.zeros_like(order).at[row_index, order].set(col_index)


def permuted(blocks, order):
    return jnp.take_along_axis(blocks, order[:, None, :], axis=2)


def swap(vector, tables):
    inv_up, order_down, inv_across, order_across = tables
    up_part = vector[:, :, :BLK]
    down_part = vector[:, :, BLK:2 * BLK]
    across = vector[:, :, 2 * BLK:]
    send_up = permuted(up_part, inv_up)
    send_down = permuted(down_part, order_down)
    parity = (jnp.arange(SUBS, dtype=jnp.int32) % 2) == 0
    send_across = jnp.where(parity[:, None, None], permuted(across, inv_across), permuted(across, order_across))
    layout = (CLUSTERS, N_SUB, SUB_DEV, LOADS, BLK)
    down_grid = send_down.reshape(layout)
    up_grid = send_up.reshape(layout)
    zero_rows = jnp.zeros_like(down_grid[:, :1])
    new_up = jnp.concatenate([down_grid[:, 1:], zero_rows], axis=1).reshape(SUBS, LOADS, BLK)
    new_down = jnp.concatenate([zero_rows, up_grid[:, :-1]], axis=1).reshape(SUBS, LOADS, BLK)
    paired = send_across.reshape(CLUSTERS, N_SUB, SUB_DEV // 2, 2, LOADS, BLK)
    even_part = paired[:, :, :, 0]
    odd_part = paired[:, :, :, 1]
    empty_part = jnp.zeros_like(even_part[:1])
    new_even = jnp.concatenate([odd_part[1:], empty_part], axis=0)
    new_odd = jnp.concatenate([empty_part, even_part[:-1]], axis=0)
    new_across = jnp.stack([new_even, new_odd], axis=3).reshape(SUBS, LOADS, BLK)
    return jnp.concatenate([new_up, new_down, new_across], axis=2)


def apply(vector, sign_field, operators, tables):
    spread = sign_field * (vector + swap(vector, tables))
    spread_bf = spread.astype(jnp.bfloat16)
    product = jnp.einsum("srk,skl->srl", spread_bf.astype(jnp.float32), operators.astype(jnp.float32), precision=HIGHEST_PRECISION)
    signed = sign_field * product
    result = signed + swap(signed, tables)
    curvature = jnp.sum(vector * result, axis=(0, 2))
    return result, curvature


def project(vector, cluster_basis, corner_basis, corner_ids, cluster_coarse, global_coarse):
    per_cluster = SUBS // CLUSTERS
    cluster_coef = jnp.einsum("srl,skl->srk", vector, cluster_basis, precision=HIGHEST_PRECISION)
    grouped = cluster_coef.reshape(CLUSTERS, per_cluster, LOADS, KC).transpose(0, 2, 1, 3).reshape(CLUSTERS, LOADS, CCO)
    solved = jnp.einsum("crm,cmn->crn", grouped, cluster_coarse, precision=HIGHEST_PRECISION)
    spread_back = solved.reshape(CLUSTERS, LOADS, per_cluster, KC).transpose(1, 0, 2, 3).reshape(LOADS, SUBS, KC)
    fix_cluster = jnp.einsum("rsk,skl->srl", spread_back, cluster_basis, precision=HIGHEST_PRECISION)
    flat_ids = corner_ids.reshape(-1).astype(jnp.int32)
    corner_coef = jnp.einsum("scl,srl->scr", corner_basis, vector, precision=HIGHEST_PRECISION).reshape(SUBS * CORN, LOADS)
    corner_sum = jax.ops.segment_sum(corner_coef, flat_ids, num_segments=NG)
    global_coef = jnp.dot(corner_sum.T, global_coarse, precision=HIGHEST_PRECISION)
    picked = jnp.take(global_coef, flat_ids, axis=1).reshape(LOADS, SUBS, CORN)
    fix_corner = jnp.einsum("rsc,scl->srl", picked, corner_basis, precision=HIGHEST_PRECISION)
    squares = jnp.sum(vector * vector, axis=(0, 2))
    return vector - fix_cluster - fix_corner, squares


def reference(rhs, operators, signs, links, cluster_basis, corner_basis, corner_ids, cluster_coarse, global_coarse):
    sign_field = signs.astype(jnp.float32)[:, None, :]
    tables = (invert(links[:, 0]), links[:, 1], invert(links[:, 2]), links[:, 2])
    residual = rhs
    projected, residual_norm = project(residual, cluster_basis, corner_basis, corner_ids, cluster_coarse, global_coarse)
    direction = projected
    multipliers = jnp.zeros_like(rhs)
    for iteration in range(ITERS):
        product, curvature = apply(direction, sign_field, operators, tables)
        step_size = (residual_norm / curvature)[None, :, None]
        multipliers = multipliers + step_size * direction
        residual = residual - step_size * product
        if iteration + 1 < ITERS:
            projected, norm_next = project(residual, cluster_basis, corner_basis, corner_ids, cluster_coarse, global_coarse)
            direction = projected + (norm_next / residual_norm)[None, :, None] * direction
            residual_norm = norm_next
    return multipliers, residual
```

```python
import functools

import jax
import jax.numpy as jnp
from jax import lax
from jax.experimental import pallas as pl
from jax.experimental.pallas import tpu as pltpu
from jax.sharding import PartitionSpec as P

ITERS = 2
LANES = 128
UNROLL = 32
MESH = pl.DeviceIdType.MESH
HIGHEST = lax.Precision.HIGHEST
NN = (((1,), (0,)), ((), ()))
NT = (((1,), (1,)), ((), ()))


def dot(a, b, dims=NN, precision=HIGHEST):
    return lax.dot_general(a, b, dims, precision=precision, preferred_element_type=jnp.float32)


def dot3(a, b, dims=NN):
    bf16, f32 = jnp.bfloat16, jnp.float32
    rows = a.shape[0]
    a_high, b_high = a.astype(bf16).astype(f32), b.astype(bf16)
    b_low = (b - b_high.astype(f32)).astype(bf16)
    halves = jnp.concatenate([a_high, a - a_high], axis=0).astype(bf16)
    out = dot(halves, b_high, dims, None)
    return out[:rows] + out[rows:] + dot(a_high.astype(bf16), b_low, dims, None)


def iota(shape, dim):
    return lax.broadcasted_iota(jnp.int32, shape, dim)


def each(count, body):
    if count <= UNROLL:
        for k in range(count):
            body(k)
    else:
        lax.fori_loop(0, count, lambda k, carry: (body(k), carry)[1], 0)


def total(ref, count, start):
    if count <= UNROLL:
        terms = [start] + [ref[k] for k in range(count)]
        while len(terms) > 1:
            terms = [sum(terms[i : i + 2][1:], terms[i]) for i in range(0, len(terms), 2)]
        return terms[0]
    return lax.fori_loop(0, count, lambda k, acc: acc + ref[k], start)


class Spread:
    def __init__(self, sizes, axes, source, slots, send, recv):
        self.sizes, self.axes = sizes, axes
        self.source, self.slots, self.send, self.recv = source, slots, send, recv
        self.count = peers_of(sizes, axes)

    def copy(self, k):
        return pltpu.make_async_remote_copy(
            src_ref=self.source,
            dst_ref=self.slots.at[k],
            send_sem=self.send.at[k],
            recv_sem=self.recv.at[k],
            device_id=peer(self.sizes, self.axes, k),
            device_id_type=MESH,
        )

    def start(self):
        each(self.count, lambda k: self.copy(k).start())

    def wait_recv(self):
        each(self.count, lambda k: self.copy(k).wait_recv())

    def wait_send(self):
        each(self.count, lambda k: self.copy(k).wait_send())


def peers_of(sizes, axes):
    clusters, members = sizes
    return {"both": clusters * members, "cluster": clusters, "sub": members}[axes] - 1


def peer(sizes, axes, k):
    clusters, members = sizes
    if axes == "both":
        c, m = (k + 1) // members, (k + 1) % members
        return {
            "cluster": lax.rem(lax.axis_index("cluster") + c, clusters),
            "sub": lax.rem(lax.axis_index("sub") + m, members),
        }
    count = clusters if axes == "cluster" else members
    return {axes: lax.rem(lax.axis_index(axes) + k + 1, count)}


def stages(sizes):
    return ("both",) if sizes[0] * sizes[1] <= UNROLL else ("cluster", "sub")


class AllSum:
    def __init__(self, sizes, refs, n):
        self.spreads = []
        for i, axes in enumerate(stages(sizes)):
            source, slots, send, recv = refs[4 * i : 4 * i + 4]
            self.spreads.append(
                Spread(sizes, axes, source.at[n], slots.at[n], send.at[n], recv.at[n])
            )

    def start(self):
        self.spreads[0].start()

    def finish(self):
        for i, spread in enumerate(self.spreads):
            spread.wait_recv()
            out = total(spread.slots, spread.count, spread.source[...])
            if i + 1 < len(self.spreads):
                self.spreads[i + 1].source[...] = out
                self.spreads[i + 1].start()
        return out

    def wait_send(self):
        for spread in self.spreads:
            spread.wait_send()


def kernel(sizes, *refs):
    clusters, members = sizes
    hbm, out_ref, refs = refs[:9], refs[9], list(refs[10:])

    def take_refs(count):
        taken = refs[:count]
        del refs[:count]
        return taken

    local_refs = take_refs(9)
    (
        rhs_ref,
        ops_ref,
        signs_ref,
        links_ref,
        cluster_basis_ref,
        corner_basis_ref,
        ids_ref,
        cluster_coarse_ref,
        global_coarse_ref,
    ) = local_refs
    (local_sem,) = take_refs(1)
    basis_ref, weights_ref, global_ref, picked_ref, swapped_basis_ref = take_refs(5)
    g_send, g_recv = take_refs(2)
    part_refs = take_refs(4)
    piece_slots, piece_send, piece_recv = take_refs(3)
    tail_refs = take_refs(4 * len(stages(sizes)))
    curve_refs = take_refs(4 * len(stages(sizes)))
    swap_refs = take_refs(8)
    table_refs = take_refs(8)

    subs, loads, dual = rhs_ref.shape
    rows = subs * loads
    kc, corn = cluster_basis_ref.shape[1], corner_basis_ref.shape[1]
    width = kc + corn
    coefs = subs * width
    order = global_coarse_ref.shape[1]
    solved = members * coefs
    my_c, my_s = lax.axis_index("cluster"), lax.axis_index("sub")
    has_low, has_high = my_s > 0, my_s < members - 1
    has_prev, has_next = my_c > 0, my_c < clusters - 1

    barrier = pltpu.get_barrier_semaphore()

    def greet(device_id):
        pl.semaphore_signal(barrier, inc=1, device_id=device_id, device_id_type=MESH)

    greeted = 0
    for axes in ("both",) if len(stages(sizes)) == 1 else ("cluster", "sub"):
        count = peers_of(sizes, axes)
        each(count, lambda k, axes=axes: greet(peer(sizes, axes, k)))
        greeted += count
    if len(stages(sizes)) > 1:
        for there, step in ((has_next, 1), (has_prev, -1)):

            @pl.when(there)
            def _():
                for m in range(1, members):
                    greet({"cluster": my_c + step, "sub": lax.rem(my_s + m, members)})

            greeted = greeted + there.astype(jnp.int32) * (members - 1)

    loads_in = [
        pltpu.make_async_copy(hbm[i], local_refs[i], local_sem.at[i]) for i in range(len(hbm))
    ]
    for i in (6, 5, 4, 0, 7, 8, 3, 2, 1):
        loads_in[i].start()
    numbers = iota((8, LANES), 1).astype(jnp.bfloat16)

    loads_in[6].wait()
    id_row = jnp.full((1, coefs), -1, jnp.int32)
    lane = iota((1, coefs), 1)
    for s in range(subs):
        for c in range(corn):
            id_row = jnp.where(lane == s * width + kc + c, ids_ref[s, c], id_row)
    id_col = jnp.sum(
        jnp.where(iota((coefs, coefs), 0) == iota((coefs, coefs), 1), id_row, 0),
        axis=1,
        keepdims=True,
    )
    weights_ref[:, solved:] = (id_col == iota((coefs, order), 1)).astype(jnp.float32)

    loads_in[5].wait()
    loads_in[4].wait()
    for s in range(subs):
        basis_ref[s * width : s * width + kc, :] = cluster_basis_ref[s]
        basis_ref[s * width + kc : (s + 1) * width, :] = corner_basis_ref[s]

    where_to = iota((1, solved), 1)
    within = lax.rem(where_to, width)
    source = (where_to // coefs) * (subs * kc) + (lax.rem(where_to, coefs) // width) * kc + within
    source = jnp.where(within < kc, source, -1)
    place = (iota((members * subs * kc, solved), 0) == source).astype(jnp.float32)
    loads_in[0].wait()
    loads_in[7].wait()
    coarse = dot(cluster_coarse_ref[0], place)
    for s in range(subs):
        weights_ref[s * width : s * width + kc, :solved] = coarse[s * kc : (s + 1) * kc]
        weights_ref[s * width + kc : (s + 1) * width, :solved] = jnp.zeros(
            (corn, solved), jnp.float32
        )

    diagonal = iota((rows, coefs), 0) // loads == iota((rows, coefs), 1) // width
    row_sub, lane_sub = iota((rows, coefs), 0) // loads, iota((rows, coefs), 1) // width
    crossed = row_sub + 1 - 2 * lax.rem(row_sub, 2) == lane_sub

    def per_load(x):
        out = x[:loads]
        for s in range(1, subs):
            out = out + x[s * loads : (s + 1) * loads]
        return out

    def lanes_added(x):
        out = x[:, :LANES]
        for b in range(1, dual // LANES):
            out = out + x[:, b * LANES : (b + 1) * LANES]
        return out

    def tiled(x):
        return jnp.concatenate([x] * subs, axis=0)

    lane_is_load = iota((loads, LANES), 0) == iota((loads, LANES), 1)

    def as_row(x):
        sums = jnp.sum(x, axis=1, keepdims=True)
        return jnp.sum(jnp.where(lane_is_load, sums, 0.0), axis=0, keepdims=True)

    def as_column(x):
        return jnp.sum(jnp.where(lane_is_load, x, 0.0), axis=1, keepdims=True)

    open_sends = []

    def piece_copy(n, side, k, step):
        target = lax.rem(my_s + k, members)
        return pltpu.make_async_remote_copy(
            src_ref=part_refs[0].at[n, target],
            dst_ref=piece_slots.at[n, side, k],
            send_sem=piece_send.at[n, side, k],
            recv_sem=piece_recv.at[n, side, k],
            device_id={"cluster": my_c + step, "sub": target},
            device_id_type=MESH,
        )

    def pieces(n, side, what):
        step = 1 - 2 * side
        for k in range(members):
            getattr(piece_copy(n, side, k, step), what)()

    def project_start(vector, n):
        raw = dot3(vector, basis_ref[...], NT)
        coef = per_load(jnp.where(diagonal, raw, 0.0))
        both = dot3(coef, weights_ref[...])
        tail_refs[0][n, :loads] = both[:, solved:]
        tail_refs[0][n, loads:, :LANES] = as_row(per_load(lanes_added(vector * vector)))
        if order > LANES:
            tail_refs[0][n, loads:, LANES:] = jnp.zeros((1, order - LANES), jnp.float32)
        for j in range(members):
            part_refs[0][n, j] = both[:, j * coefs : (j + 1) * coefs]

    def project_send(n):
        tail = AllSum(sizes, tail_refs, n)
        tail.start()
        part = Spread(sizes, "sub", *[ref.at[n] for ref in part_refs])
        part.start()
        pl.when(has_next)(lambda: pieces(n, 0, "start"))
        pl.when(has_prev)(lambda: pieces(n, 1, "start"))
        return tail, part

    def project_finish(n, tail, part):
        part.wait_recv()
        pl.when(has_prev)(lambda: pieces(n, 0, "wait_recv"))
        pl.when(has_next)(lambda: pieces(n, 1, "wait_recv"))

        def cluster_of(member):
            out = part_refs[0][n, member]
            for k in range(members - 1):
                out = out + part_refs[1][n, k, member]
            return out

        def piece_sum(side):
            return total(piece_slots.at[n, side], members - 1, piece_slots[n, side, members - 1])

        own = cluster_of(my_s)
        high = cluster_of(jnp.minimum(my_s + 1, members - 1))
        low = cluster_of(jnp.maximum(my_s - 1, 0))
        prev, following = piece_sum(0), piece_sum(1)
        summed = tail.finish()
        open_sends.extend([tail, part])
        norm = as_column(summed[loads:, :LANES])
        corners = dot3(summed[:loads], picked_ref[...])

        def amount(base, i):
            return base + corners[:, i * coefs : (i + 1) * coefs]

        def block_diagonal(x, mask):
            return jnp.where(mask, tiled(x), 0.0)

        fix = dot3(block_diagonal(amount(own, 0), diagonal), basis_ref[...])
        high = jnp.where(has_high, amount(high, 1), 0.0)
        low = jnp.where(has_low, amount(low, 2), 0.0)
        following = jnp.where(has_next, amount(following, 3), 0.0)
        prev = jnp.where(has_prev, amount(prev, 4), 0.0)
        odd = lax.rem(iota((loads, coefs), 1) // width, 2) == 1
        cross = jnp.where(odd, following, prev)
        fix_swapped = jnp.concatenate(
            [
                dot3(block_diagonal(high, diagonal), swapped_basis_ref[0]),
                dot3(block_diagonal(low, diagonal), swapped_basis_ref[1]),
                dot3(block_diagonal(cross, crossed), swapped_basis_ref[2]),
            ],
            axis=1,
        )
        return fix, fix_swapped, norm

    def take(x, order_of):
        return jnp.take_along_axis(x, order_of, axis=1, mode="promise_in_bounds")

    class Swap:
        def __init__(self, refs, n):
            in_src, in_slots, in_send, in_recv, out_src, out_slots, out_send, out_recv = refs
            self.sources = [in_src.at[n, 0], in_src.at[n, 1], out_src.at[n, 0], out_src.at[n, 1]]
            self.slots = [
                in_slots.at[n, 0],
                in_slots.at[n, 1],
                out_slots.at[n, 0],
                out_slots.at[n, 1],
            ]
            self.send = [in_send.at[n, 0], in_send.at[n, 1], out_send.at[n, 0], out_send.at[n, 1]]
            self.recv = [in_recv.at[n, 0], in_recv.at[n, 1], out_recv.at[n, 0], out_recv.at[n, 1]]
            self.sends = [has_high, has_low, has_next, has_prev]
            self.takes = [has_low, has_high, has_prev, has_next]

        def copy(self, i):
            axis = "sub" if i < 2 else "cluster"
            return pltpu.make_async_remote_copy(
                src_ref=self.sources[i],
                dst_ref=self.slots[i],
                send_sem=self.send[i],
                recv_sem=self.recv[i],
                device_id={axis: lax.axis_index(axis) + (-1 if i % 2 else 1)},
                device_id_type=MESH,
            )

        def start(self, x, orders, height, extra=None):
            up_order, down_order, across_order = orders
            count = subs * height
            across = take(x[:, 2 * LANES :], across_order)
            for p in range(2):
                for h in range(subs // 2):
                    s = 2 * h + p
                    self.sources[2 + p][h * height : (h + 1) * height] = across[
                        s * height : (s + 1) * height
                    ]
            self.sources[0][:count] = take(x[:, :LANES], up_order)
            self.sources[1][:count] = take(x[:, LANES : 2 * LANES], down_order)
            if extra is not None:
                for i in range(4):
                    first = count if i < 2 else count // 2
                    self.sources[i][first : first + 8] = extra
            for i in (2, 3, 0, 1):
                pl.when(self.sends[i])(self.copy(i).start)

        def wait_recv(self):
            for i in range(4):
                pl.when(self.takes[i])(self.copy(i).wait_recv)

        def wait_send(self):
            for i in range(4):
                pl.when(self.sends[i])(self.copy(i).wait_send)

        def arrived(self, i):
            return jnp.where(self.takes[i], self.slots[i][...], 0.0)

        def field(self):
            self.wait_recv()
            at_odd, at_even = self.arrived(2), self.arrived(3)
            across = [
                (at_odd if s % 2 else at_even)[s // 2 * loads : (s // 2 + 1) * loads]
                for s in range(subs)
            ]
            return jnp.concatenate(
                [self.arrived(1), self.arrived(0), jnp.concatenate(across, axis=0)], axis=1
            )

    depth = global_coarse_ref.shape[0]
    own_rows = pl.ds(pl.multiple_of(my_s * depth, 8), depth)

    def gather_copy(k):
        return pltpu.make_async_remote_copy(
            src_ref=global_coarse_ref,
            dst_ref=global_ref.at[own_rows],
            send_sem=g_send.at[k],
            recv_sem=g_recv.at[k],
            device_id=peer(sizes, "sub", k),
            device_id_type=MESH,
        )

    def begin():
        loads_in[8].wait()
        global_ref[own_rows, :] = global_coarse_ref[...]
        each(members - 1, lambda k: gather_copy(k).start())
        loads_in[3].wait()

        def plain(row):
            return row

        def inverted(row):
            hot = (iota((LANES, LANES), 0) == row).astype(jnp.float32).astype(jnp.bfloat16)
            return dot(numbers, hot, NT, None)[:1].astype(jnp.int32)

        index = [
            [inverted(links_ref[0, s : s + 1, :]) for s in range(subs)],
            [plain(links_ref[1, s : s + 1, :]) for s in range(subs)],
            [(plain if s % 2 else inverted)(links_ref[2, s : s + 1, :]) for s in range(subs)],
        ]

        def orders_of(height):
            return [
                jnp.concatenate(
                    [jnp.broadcast_to(row, (height, LANES)) for row in block], axis=0
                )
                for block in index
            ]

        orders = orders_of(loads)
        rhs_swap = Swap(swap_refs, ITERS)
        rhs_swap.start(rhs, orders, loads)
        tables = Swap(table_refs, 0)
        ids_sent = jnp.broadcast_to(id_row.astype(jnp.float32), (8, coefs))
        tables.start(basis_ref[...], orders_of(width), width, ids_sent)

        loads_in[2].wait()
        sign = jnp.concatenate(
            [
                jnp.broadcast_to(signs_ref[s : s + 1, :].astype(jnp.float32), (loads, dual))
                for s in range(subs)
            ],
            axis=0,
        )
        each(members - 1, lambda k: gather_copy(k).wait_recv())
        tables.wait_recv()
        swapped_basis_ref[0] = tables.arrived(1)[:coefs]
        swapped_basis_ref[1] = tables.arrived(0)[:coefs]
        from_prev, from_next = tables.arrived(2), tables.arrived(3)
        for s in range(subs):
            swapped_basis_ref[2, s * width : (s + 1) * width] = (
                from_next if s % 2 else from_prev
            )[s // 2 * width : (s // 2 + 1) * width]
        id_rows = [id_row.astype(jnp.float32)]
        for i in (1, 0, 3, 2):
            first = coefs if i < 2 else coefs // 2
            id_rows.append(tables.slots[i][first : first + 1])
        whose = iota((order, coefs), 0).astype(jnp.float32)
        picks = jnp.concatenate([(row == whose).astype(jnp.float32) for row in id_rows], axis=1)
        for r in range(0, order, 2 * LANES):
            chunk = slice(r, min(r + 2 * LANES, order))
            picked_ref[chunk] = dot(global_ref[chunk], picks)
        loads_in[1].wait()
        open_sends.extend([rhs_swap, tables])
        return sign, orders, rhs_swap.field()

    rhs = jnp.concatenate([rhs_ref[s] for s in range(subs)], axis=0)
    project_start(rhs, 0)
    pl.semaphore_wait(barrier, greeted)
    started = project_send(0)
    sign, orders, residual_swapped = begin()
    fix, fix_swapped, rho = project_finish(0, *started)
    residual = rhs
    direction, direction_swapped = residual - fix, residual_swapped - fix_swapped
    row_odd = lax.rem(iota((rows, LANES), 0) // loads, 2) == 1
    there = jnp.concatenate(
        [
            jnp.full((rows, LANES), has_high.astype(jnp.float32)),
            jnp.full((rows, LANES), has_low.astype(jnp.float32)),
            jnp.where(row_odd, has_prev.astype(jnp.float32), has_next.astype(jnp.float32)),
        ],
        axis=1,
    )
    multipliers = None
    for n in range(ITERS):
        spread = sign * (direction + direction_swapped)
        spread_bf = spread.astype(jnp.bfloat16)
        image = jnp.concatenate(
            [
                dot(spread_bf[s * loads : (s + 1) * loads], ops_ref[s], NN, None)
                for s in range(subs)
            ],
            axis=0,
        )
        curve_refs[0][n] = as_row(per_load(lanes_added(spread * image)))
        curve = AllSum(sizes, curve_refs, n)
        curve.start()
        signed = sign * image
        swap = Swap(swap_refs, n)
        swap.start(signed, orders, loads)
        signed_swapped = swap.field()
        product = signed + signed_swapped
        product_swapped = signed_swapped + there * signed
        curvature = as_column(curve.finish())
        open_sends.extend([curve, swap])
        step = tiled(rho / curvature)
        residual = residual - step * product
        if n + 1 < ITERS:
            project_start(residual, n + 1)
            started = project_send(n + 1)
        moved = step * direction
        multipliers = moved if multipliers is None else multipliers + moved
        if n + 1 < ITERS:
            residual_swapped = residual_swapped - step * product_swapped
            fix, fix_swapped, rho_new = project_finish(n + 1, *started)
            ratio = tiled(rho_new / rho)
            direction = residual - fix + ratio * direction
            direction_swapped = residual_swapped - fix_swapped + ratio * direction_swapped
            rho = rho_new
    for s in range(subs):
        out_ref[0, s] = multipliers[s * loads : (s + 1) * loads]
        out_ref[1, s] = residual[s * loads : (s + 1) * loads]
    for spread in open_sends:
        spread.wait_send()
    each(members - 1, lambda k: gather_copy(k).wait_send())
    for n in range(ITERS):
        pl.when(has_next)(lambda n=n: pieces(n, 0, "wait_send"))
        pl.when(has_prev)(lambda n=n: pieces(n, 1, "wait_send"))


def split(both_ref, mult_ref, res_ref, sems):
    copies = [
        pltpu.make_async_copy(both_ref.at[i], out, sems.at[i])
        for i, out in enumerate((mult_ref, res_ref))
    ]
    for copy in copies:
        copy.start()
    for copy in copies:
        copy.wait()


def local(sizes, *args):
    args = list(args)
    args[3] = jnp.transpose(args[3], (1, 0, 2))
    rhs, operators, signs, links, cluster_basis, corner_basis, ids, coarse, glob = args
    clusters, members = sizes
    subs, loads, dual = rhs.shape
    coefs = subs * (cluster_basis.shape[1] + corner_basis.shape[1])
    depth, order = glob.shape
    f32 = jnp.float32
    dma = pltpu.SemaphoreType.DMA

    def exchange(lead, block, receive):
        return [
            pltpu.VMEM(lead[:1] + block, f32),
            pltpu.VMEM(lead + receive, f32),
            dma(lead),
            dma(lead),
        ]

    def swap_scratch(count, height, extra):
        scratch = []
        for rows in (subs * height + extra, subs * height // 2 + extra):
            scratch += [
                pltpu.VMEM((count, 2, rows, LANES), f32),
                pltpu.VMEM((count, 2, rows, LANES), f32),
                dma((count, 2)),
                dma((count, 2)),
            ]
        return scratch

    def sum_scratch(block):
        scratch = []
        for axes in stages(sizes):
            scratch += exchange((ITERS, peers_of(sizes, axes)), block, block)
        return scratch

    vmem = pl.BlockSpec(memory_space=pltpu.VMEM)
    scratch = [pltpu.VMEM(a.shape, a.dtype) for a in args]
    scratch[6] = pltpu.SMEM(ids.shape, ids.dtype)
    scratch += [
        dma((len(args),)),
        pltpu.VMEM((coefs, dual), f32),
        pltpu.VMEM((coefs, members * coefs + order), f32),
        pltpu.VMEM((order, order), f32),
        pltpu.VMEM((order, 5 * coefs), f32),
        pltpu.VMEM((3, coefs, LANES), f32),
        dma((members - 1,)),
        dma((members - 1,)),
    ]
    part = (members, loads, coefs)
    scratch += exchange((ITERS, members - 1), part, part)
    scratch += [
        pltpu.VMEM((ITERS, 2, members, loads, coefs), f32),
        dma((ITERS, 2, members)),
        dma((ITERS, 2, members)),
    ]
    scratch += sum_scratch((loads + 1, order)) + sum_scratch((1, LANES))
    scratch += swap_scratch(ITERS + 1, loads, 0)
    scratch += swap_scratch(1, coefs // subs, 8)
    both = pl.pallas_call(
        functools.partial(kernel, sizes),
        out_shape=pltpu.VMEM((2,) + rhs.shape, f32),
        in_specs=[pl.BlockSpec(memory_space=pltpu.HBM)] * len(args),
        out_specs=vmem,
        scratch_shapes=scratch,
        compiler_params=pltpu.CompilerParams(
            collective_id=0, has_side_effects=True, vmem_limit_bytes=56 << 20
        ),
    )(*args)
    return pl.pallas_call(
        split,
        out_shape=[jax.ShapeDtypeStruct(rhs.shape, f32)] * 2,
        in_specs=[vmem],
        out_specs=[pl.BlockSpec(memory_space=pltpu.HBM)] * 2,
        scratch_shapes=[dma((2,))],
        compiler_params=pltpu.CompilerParams(vmem_limit_bytes=4 << 20),
    )(both)


def solution(mesh):
    placed = (
        P(("cluster", "sub"), None, None),
        P(("cluster", "sub"), None, None),
        P(("cluster", "sub"), None),
        P(("cluster", "sub"), None, None),
        P(("cluster", "sub"), None, None),
        P(("cluster", "sub"), None, None),
        P(("cluster", "sub"), None),
        P("cluster", "sub", None),
        P("sub", None),
    )
    return jax.shard_map(
        functools.partial(local, (mesh.shape["cluster"], mesh.shape["sub"])),
        mesh=mesh,
        in_specs=placed,
        out_specs=(P(("cluster", "sub"), None, None), P(("cluster", "sub"), None, None)),
        check_vma=False,
    )
```

```python
import functools

import jax
import jax.numpy as jnp
from jax import lax
from jax.experimental import pallas as pl
from jax.experimental.pallas import tpu as pltpu
from jax.sharding import PartitionSpec as P

ITERS = 2
LANES = 128
UNROLL = 32
MESH = pl.DeviceIdType.MESH
HIGHEST = lax.Precision.HIGHEST
NN = (((1,), (0,)), ((), ()))
NT = (((1,), (1,)), ((), ()))


def dot(a, b, dims=NN, precision=HIGHEST):
    return lax.dot_general(a, b, dims, precision=precision, preferred_element_type=jnp.float32)


def halves(x):
    high = x.astype(jnp.bfloat16)
    return high, (x - high.astype(jnp.float32)).astype(jnp.bfloat16)


def stacked(a):
    high = a.astype(jnp.bfloat16).astype(jnp.float32)
    return jnp.concatenate([high, a - high], axis=0).astype(jnp.bfloat16), high.astype(jnp.bfloat16)


def dot2(a, b, dims=NN):
    rows = a.shape[0]
    out = dot(stacked(a)[0], b, dims, None)
    return out[:rows] + out[rows:]


def dot3(a, b, dims=NN):
    rows = a.shape[0]
    both, high = stacked(a)
    out = dot(both, b[0], dims, None)
    return out[:rows] + out[rows:] + dot(high, b[1], dims, None)


def put(ref, index, x):
    for i, half in enumerate(halves(x)):
        ref[(i,) + index] = half


def iota(shape, dim):
    return lax.broadcasted_iota(jnp.int32, shape, dim)


def each(count, body):
    if count <= UNROLL:
        for k in range(count):
            body(k)
    else:
        lax.fori_loop(0, count, lambda k, carry: (body(k), carry)[1], 0)


def total(ref, count, start):
    if count <= UNROLL:
        terms = [start] + [ref[k] for k in range(count)]
        while len(terms) > 1:
            terms = [sum(terms[i : i + 2][1:], terms[i]) for i in range(0, len(terms), 2)]
        return terms[0]
    return lax.fori_loop(0, count, lambda k, acc: acc + ref[k], start)


class Spread:
    def __init__(self, sizes, axes, source, slots, send, recv):
        self.sizes, self.axes = sizes, axes
        self.source, self.slots, self.send, self.recv = source, slots, send, recv
        self.count = peers_of(sizes, axes)

    def copy(self, k):
        return pltpu.make_async_remote_copy(
            src_ref=self.source,
            dst_ref=self.slots.at[k],
            send_sem=self.send.at[k],
            recv_sem=self.recv.at[k],
            device_id=peer(self.sizes, self.axes, k),
            device_id_type=MESH,
        )

    def start(self):
        each(self.count, lambda k: self.copy(k).start())

    def wait_recv(self):
        each(self.count, lambda k: self.copy(k).wait_recv())

    def wait_send(self):
        each(self.count, lambda k: self.copy(k).wait_send())


def peers_of(sizes, axes):
    clusters, members = sizes
    return {"both": clusters * members, "cluster": clusters, "sub": members}[axes] - 1


def peer(sizes, axes, k):
    clusters, members = sizes
    if axes == "both":
        c, m = (k + 1) // members, (k + 1) % members
        return {
            "cluster": lax.rem(lax.axis_index("cluster") + c, clusters),
            "sub": lax.rem(lax.axis_index("sub") + m, members),
        }
    count = clusters if axes == "cluster" else members
    return {axes: lax.rem(lax.axis_index(axes) + k + 1, count)}


def stages(sizes):
    return ("both",) if sizes[0] * sizes[1] <= UNROLL else ("cluster", "sub")


class AllSum:
    def __init__(self, sizes, refs, n):
        self.spreads = []
        for i, axes in enumerate(stages(sizes)):
            source, slots, send, recv = refs[4 * i : 4 * i + 4]
            self.spreads.append(
                Spread(sizes, axes, source.at[n], slots.at[n], send.at[n], recv.at[n])
            )

    def start(self):
        self.spreads[0].start()

    def finish(self):
        for i, spread in enumerate(self.spreads):
            spread.wait_recv()
            out = total(spread.slots, spread.count, spread.source[...])
            if i + 1 < len(self.spreads):
                self.spreads[i + 1].source[...] = out
                self.spreads[i + 1].start()
        return out

    def wait_send(self):
        for spread in self.spreads:
            spread.wait_send()


def kernel(sizes, *refs):
    clusters, members = sizes
    hbm, out_ref, refs = refs[:9], refs[9], list(refs[10:])

    def take_refs(count):
        taken = refs[:count]
        del refs[:count]
        return taken

    local_refs = take_refs(9)
    (
        rhs_ref,
        ops_ref,
        signs_ref,
        links_ref,
        cluster_basis_ref,
        corner_basis_ref,
        ids_ref,
        cluster_coarse_ref,
        global_coarse_ref,
    ) = local_refs
    (local_sem,) = take_refs(1)
    basis_ref, basis_halves, swapped_basis, solve_ref, hot_ref = take_refs(5)
    global_ref, picked_ref = take_refs(2)
    g_send, g_recv = take_refs(2)
    near_coarse, near_send, near_recv = take_refs(3)
    cross_refs = take_refs(4)
    (share_ref,) = take_refs(1)
    share_refs = [take_refs(3) for _ in range(2)]
    tail_refs = take_refs(4 * len(stages(sizes)))
    curve_refs = take_refs(4 * len(stages(sizes)))
    swap_refs = take_refs(8)
    table_refs = take_refs(8)

    subs, loads, dual = rhs_ref.shape
    rows = subs * loads
    kc, corn = cluster_basis_ref.shape[1], corner_basis_ref.shape[1]
    width = kc + corn
    coefs = subs * width
    order = global_coarse_ref.shape[1]
    solved = members * coefs
    near = share_refs[0][0].shape[2]
    my_c, my_s = lax.axis_index("cluster"), lax.axis_index("sub")
    has_low, has_high = my_s > 0, my_s < members - 1
    has_prev, has_next = my_c > 0, my_c < clusters - 1

    barrier = pltpu.get_barrier_semaphore()

    def greet(device_id):
        pl.semaphore_signal(barrier, inc=1, device_id=device_id, device_id_type=MESH)

    greeted = 0
    for axes in ("both",) if len(stages(sizes)) == 1 else ("cluster", "sub"):
        count = peers_of(sizes, axes)
        each(count, lambda k, axes=axes: greet(peer(sizes, axes, k)))
        greeted += count
    if len(stages(sizes)) > 1:
        for there, step in ((has_next, 1), (has_prev, -1)):

            @pl.when(there)
            def _():
                for m in range(1, members):
                    greet({"cluster": my_c + step, "sub": lax.rem(my_s + m, members)})

            greeted = greeted + there.astype(jnp.int32) * (members - 1)

    loads_in = [
        pltpu.make_async_copy(hbm[i], local_refs[i], local_sem.at[i]) for i in range(len(hbm))
    ]
    for i in (6, 5, 4, 0, 7, 8, 3, 2, 1):
        loads_in[i].start()
    numbers = iota((8, LANES), 1).astype(jnp.bfloat16)

    loads_in[6].wait()
    id_row = jnp.full((1, coefs), -1, jnp.int32)
    lane = iota((1, coefs), 1)
    for s in range(subs):
        for c in range(corn):
            id_row = jnp.where(lane == s * width + kc + c, ids_ref[s, c], id_row)
    whose = iota((order, coefs), 0).astype(jnp.float32)
    corner_of = iota((coefs, order), 1).astype(jnp.float32)

    def hot_of(row):
        return (row == whose).astype(jnp.float32)

    def put_hot(i, row):
        same = iota((coefs, coefs), 0) == iota((coefs, coefs), 1)
        column = jnp.sum(jnp.where(same, row, 0.0), axis=1, keepdims=True)
        hot = (column == corner_of).astype(jnp.float32)
        hot_ref[i * coefs : (i + 1) * coefs] = hot.astype(jnp.bfloat16)

    put_hot(0, id_row.astype(jnp.float32))

    loads_in[5].wait()
    loads_in[4].wait()
    for s in range(subs):
        basis_ref[s * width : s * width + kc, :] = cluster_basis_ref[s]
        basis_ref[s * width + kc : (s + 1) * width, :] = corner_basis_ref[s]
    put(basis_halves, (), basis_ref[...])

    where_to = iota((1, solved), 1)
    within = lax.rem(where_to, width)
    source = (where_to // coefs) * (subs * kc) + (lax.rem(where_to, coefs) // width) * kc + within
    source = jnp.where(within < kc, source, -1)
    place = (iota((members * subs * kc, solved), 0) == source).astype(jnp.float32)
    place = place.astype(jnp.bfloat16)

    def placed(x):
        return [dot(half, place, NN, None).astype(jnp.bfloat16) for half in halves(x)]

    solve_ref[...] = jnp.zeros(solve_ref.shape, jnp.bfloat16)

    def put_solve(first, x):
        for i, half in enumerate(placed(x)):
            for s in range(subs):
                at = first + s * width
                solve_ref[i, at : at + kc] = half[s * kc : (s + 1) * kc]

    loads_in[0].wait()
    loads_in[7].wait()
    put_solve(0, cluster_coarse_ref[0])

    diagonal = iota((rows, coefs), 0) // loads == iota((rows, coefs), 1) // width
    row_sub, lane_sub = iota((rows, coefs), 0) // loads, iota((rows, coefs), 1) // width
    crossed = row_sub + 1 - 2 * lax.rem(row_sub, 2) == lane_sub
    image_sub = iota((rows, dual), 0) // loads

    def per_load(x):
        out = x[:loads]
        for s in range(1, subs):
            out = out + x[s * loads : (s + 1) * loads]
        return out

    def lanes_added(x):
        out = x[:, :LANES]
        for b in range(1, dual // LANES):
            out = out + x[:, b * LANES : (b + 1) * LANES]
        return out

    def tiled(x):
        return jnp.concatenate([x] * subs, axis=0)

    def as_row(x):
        shape = (x.shape[0], LANES)
        sums = jnp.sum(x, axis=1, keepdims=True)
        kept = jnp.where(iota(shape, 0) == iota(shape, 1), sums, 0.0)
        return jnp.sum(kept, axis=0, keepdims=True)

    def as_column(x, first=0):
        mine = iota((rows, LANES), 1) == lax.rem(iota((rows, LANES), 0), loads) + first
        return jnp.sum(jnp.where(mine, x, 0.0), axis=1, keepdims=True)

    def dots(*products):
        return as_row(jnp.concatenate([per_load(lanes_added(x)) for x in products], axis=0))

    open_sends = []

    def first_near(member):
        return jnp.clip(member - 1, 0, members - near)

    def near_part(ref, target):
        return ref.at[pl.ds(first_near(target), near)]

    def push(refs, at, source, step, target):
        slots, send, recv = refs
        device_id = {"sub": target}
        if step:
            device_id["cluster"] = my_c + step
        return pltpu.make_async_remote_copy(
            src_ref=source,
            dst_ref=slots.at[at],
            send_sem=send.at[at],
            recv_sem=recv.at[at],
            device_id=device_id,
            device_id_type=MESH,
        )

    class Shares:
        def __init__(self, n):
            own, pieces = share_refs
            self.n = n
            mine = share_ref.at[n]

            def target(k):
                return lax.rem(my_s + k, members)

            def copies(refs, lead, of, step, ks):
                return lambda: [
                    push(refs, lead + (k,), of(target(k)), step, target(k)) for k in ks
                ]

            near_mine = functools.partial(near_part, mine)
            self.groups = [(None, None, copies(own, (n,), near_mine, 0, range(1, members)))]
            for side, sends, takes in ((0, has_next, has_prev), (1, has_prev, has_next)):
                make = copies(
                    pieces, (n, side), lambda t: mine.at[t], 1 - 2 * side, range(members)
                )
                self.groups.append((sends, takes, make))

        def run(self, what):
            for sends, takes, make in self.groups:
                when = takes if what == "wait_recv" else sends

                def act(make=make):
                    for copy in make():
                        getattr(copy, what)()

                act() if when is None else pl.when(when)(act)

        def start(self):
            self.run("start")

        def wait_send(self):
            self.run("wait_send")

        def solutions(self):
            self.run("wait_recv")
            n = self.n
            own, pieces = [refs[0] for refs in share_refs]
            base = first_near(my_s)

            def sum_of(terms):
                while len(terms) > 1:
                    terms = [sum(terms[i : i + 2][1:], terms[i]) for i in range(0, len(terms), 2)]
                return terms[0]

            def of_member(member):
                near_slots = [own[n, k, member - base] for k in range(1, members)]
                return sum_of([share_ref[n, member]] + near_slots)

            def of_side(side):
                return sum_of([pieces[n, side, k] for k in range(members)])

            high = of_member(jnp.minimum(my_s + 1, members - 1))
            low = of_member(jnp.maximum(my_s - 1, 0))
            return [of_member(my_s), high, low, of_side(1), of_side(0)]

    def sums(n, raw, row):
        tail_refs[0][n, :loads] = dot2(
            jnp.concatenate(raw, axis=1), hot_ref[: len(raw) * coefs]
        )
        tail_refs[0][n, loads:, :LANES] = row
        if order > LANES:
            tail_refs[0][n, loads:, LANES:] = jnp.zeros((1, order - LANES), jnp.float32)
        tail = AllSum(sizes, tail_refs, n)
        share = Shares(n)

        def solve():
            share_out(n, jnp.concatenate(raw[:3], axis=1))

        return tail, share, solve

    def share_out(n, inside):
        out = dot3(inside, [solve_ref[i, : inside.shape[1]] for i in range(2)])
        for j in range(members):
            share_ref[n, j] = out[:, j * coefs : (j + 1) * coefs]

    def block_diagonal(x, mask):
        return jnp.where(mask, tiled(x), 0.0)

    def raw_of(halved, lanes, b, mask):
        both, high = halved
        out = dot(both[:, lanes], b[0], NT, None)
        x = out[:rows] + out[rows:] + dot(high[:, lanes], b[1], NT, None)
        return per_load(jnp.where(mask, x, 0.0))

    def own_raw(halved):
        return raw_of(halved, slice(0, dual), basis_halves, diagonal)

    def swapped_raw(halved, i):
        lanes = slice(i * LANES, (i + 1) * LANES)
        b = [swapped_basis[0, i], swapped_basis[1, i]]
        return raw_of(halved, lanes, b, crossed if i == 2 else diagonal)

    def correction(tail, shares):
        own, high, low, following, prev = shares[0].solutions()
        summed = tail.finish()
        open_sends.extend([tail] + shares)
        corners = dot3(summed[:loads], picked_ref)
        for share in shares[1:]:
            late = share.solutions()
            own, high, low, following, prev = [
                a + b for a, b in zip((own, high, low, following, prev), late)
            ]

        def amount(base, i):
            return base + corners[:, i * coefs : (i + 1) * coefs]

        fix = dot3(block_diagonal(amount(own, 0), diagonal), basis_halves)
        high = jnp.where(has_high, amount(high, 1), 0.0)
        low = jnp.where(has_low, amount(low, 2), 0.0)
        following = jnp.where(has_next, amount(following, 3), 0.0)
        prev = jnp.where(has_prev, amount(prev, 4), 0.0)
        odd = lax.rem(iota((loads, coefs), 1) // width, 2) == 1
        cross = jnp.where(odd, following, prev)
        parts = ((high, diagonal), (low, diagonal), (cross, crossed))
        fix_swapped = jnp.concatenate(
            [
                dot3(block_diagonal(x, mask), [swapped_basis[0, i], swapped_basis[1, i]])
                for i, (x, mask) in enumerate(parts)
            ],
            axis=1,
        )
        return fix, fix_swapped, summed[loads:, :LANES]

    def image_of(spread):
        out = None
        for s in range(subs):
            x = dot(spread, ops_ref[s], NN, None)
            if x.shape[0] > rows:
                x = x[:rows] + x[rows:]
            out = x if out is None else jnp.where(image_sub == s, x, out)
        return out

    def take(x, order_of):
        return jnp.take_along_axis(x, order_of, axis=1, mode="promise_in_bounds")

    class Swap:
        def __init__(self, refs, n):
            in_src, in_slots, in_send, in_recv, out_src, out_slots, out_send, out_recv = refs
            self.sources = [in_src.at[n, 0], in_src.at[n, 1], out_src.at[n, 0], out_src.at[n, 1]]
            self.slots = [
                in_slots.at[n, 0],
                in_slots.at[n, 1],
                out_slots.at[n, 0],
                out_slots.at[n, 1],
            ]
            self.send = [in_send.at[n, 0], in_send.at[n, 1], out_send.at[n, 0], out_send.at[n, 1]]
            self.recv = [in_recv.at[n, 0], in_recv.at[n, 1], out_recv.at[n, 0], out_recv.at[n, 1]]
            self.sends = [has_high, has_low, has_next, has_prev]
            self.takes = [has_low, has_high, has_prev, has_next]

        def copy(self, i):
            axis = "sub" if i < 2 else "cluster"
            return pltpu.make_async_remote_copy(
                src_ref=self.sources[i],
                dst_ref=self.slots[i],
                send_sem=self.send[i],
                recv_sem=self.recv[i],
                device_id={axis: lax.axis_index(axis) + (-1 if i % 2 else 1)},
                device_id_type=MESH,
            )

        def fill(self, x, orders, height, extra=None):
            up_order, down_order, across_order = orders
            count = subs * height
            across = take(x[:, 2 * LANES :], across_order)
            for p in range(2):
                for h in range(subs // 2):
                    s = 2 * h + p
                    self.sources[2 + p][h * height : (h + 1) * height] = across[
                        s * height : (s + 1) * height
                    ]
            self.sources[0][:count] = take(x[:, :LANES], up_order)
            self.sources[1][:count] = take(x[:, LANES : 2 * LANES], down_order)
            if extra is not None:
                for i in range(4):
                    first = count if i < 2 else count // 2
                    self.sources[i][first : first + 8] = extra

        def start(self):
            for i in (2, 3, 0, 1):
                pl.when(self.sends[i])(self.copy(i).start)

        def wait_recv(self):
            for i in range(4):
                pl.when(self.takes[i])(self.copy(i).wait_recv)

        def wait_send(self):
            for i in range(4):
                pl.when(self.sends[i])(self.copy(i).wait_send)

        def arrived(self, i):
            return jnp.where(self.takes[i], self.slots[i][...], 0.0)

        def field(self):
            self.wait_recv()
            at_odd, at_even = self.arrived(2), self.arrived(3)
            across = [
                (at_odd if s % 2 else at_even)[s // 2 * loads : (s // 2 + 1) * loads]
                for s in range(subs)
            ]
            return jnp.concatenate(
                [self.arrived(1), self.arrived(0), jnp.concatenate(across, axis=0)], axis=1
            )

    depth = global_coarse_ref.shape[0]
    own_rows = pl.ds(pl.multiple_of(my_s * depth, 8), depth)

    def gather_copy(k):
        return pltpu.make_async_remote_copy(
            src_ref=global_coarse_ref,
            dst_ref=global_ref.at[own_rows],
            send_sem=g_send.at[k],
            recv_sem=g_recv.at[k],
            device_id=peer(sizes, "sub", k),
            device_id_type=MESH,
        )

    def near_copy(slot):
        return pltpu.make_async_remote_copy(
            src_ref=cluster_coarse_ref.at[0],
            dst_ref=near_coarse.at[slot],
            send_sem=near_send.at[slot],
            recv_sem=near_recv.at[slot],
            device_id={"sub": my_s + (1 if slot else -1)},
            device_id_type=MESH,
        )

    def cross_copy(slot):
        return pltpu.make_async_remote_copy(
            src_ref=cross_refs[0],
            dst_ref=cross_refs[1].at[slot],
            send_sem=cross_refs[2].at[slot],
            recv_sem=cross_refs[3].at[slot],
            device_id={"cluster": my_c + (-1 if slot else 1)},
            device_id_type=MESH,
        )

    coarse_sends = (
        (has_low, has_high, lambda: [near_copy(0)]),
        (has_high, has_low, lambda: [near_copy(1)]),
    )

    def coarse_run(what):
        for sends, takes, make in coarse_sends:

            def act(make=make):
                for copy in make():
                    getattr(copy, what)()

            pl.when(takes if what == "wait_recv" else sends)(act)

    def plain(row):
        return row

    def inverted(row):
        hot = (iota((LANES, LANES), 0) == row).astype(jnp.float32).astype(jnp.bfloat16)
        return dot(numbers, hot, NT, None)[:1].astype(jnp.int32)

    loads_in[3].wait()
    index = [
        [inverted(links_ref[0, s : s + 1, :]) for s in range(subs)],
        [plain(links_ref[1, s : s + 1, :]) for s in range(subs)],
        [(plain if s % 2 else inverted)(links_ref[2, s : s + 1, :]) for s in range(subs)],
    ]

    def orders_of(height):
        return [
            jnp.concatenate([jnp.broadcast_to(row, (height, LANES)) for row in block], axis=0)
            for block in index
        ]

    rhs = jnp.concatenate([rhs_ref[s] for s in range(subs)], axis=0)
    orders = orders_of(loads)
    rhs_swap, tables = Swap(swap_refs, ITERS), Swap(table_refs, 0)
    rhs_swap.fill(rhs, orders, loads)
    ids_sent = jnp.broadcast_to(id_row.astype(jnp.float32), (8, coefs))
    tables.fill(basis_ref[...], orders_of(width), width, ids_sent)
    tail, share, solve = sums(0, [own_raw(stacked(rhs))], dots(rhs * rhs))
    solve()
    loads_in[8].wait()
    global_ref[own_rows, :] = global_coarse_ref[...]
    pl.semaphore_wait(barrier, greeted)
    tail.start()
    share.start()
    tables.start()
    each(members - 1, lambda k: gather_copy(k).start())
    rhs_swap.start()
    coarse_run("start")

    loads_in[2].wait()
    sign = jnp.concatenate(
        [
            jnp.broadcast_to(signs_ref[s : s + 1, :].astype(jnp.float32), (loads, dual))
            for s in range(subs)
        ],
        axis=0,
    )
    row_odd = lax.rem(iota((rows, LANES), 0) // loads, 2) == 1
    there = jnp.concatenate(
        [
            jnp.full((rows, LANES), has_high.astype(jnp.float32)),
            jnp.full((rows, LANES), has_low.astype(jnp.float32)),
            jnp.where(row_odd, has_prev.astype(jnp.float32), has_next.astype(jnp.float32)),
        ],
        axis=1,
    )
    loads_in[1].wait()
    open_sends.extend([rhs_swap, tables])
    each(members - 1, lambda k: gather_copy(k).wait_recv())
    tables.wait_recv()
    put(swapped_basis, (0,), tables.arrived(1)[:coefs])
    put(swapped_basis, (1,), tables.arrived(0)[:coefs])
    from_prev, from_next = tables.arrived(2), tables.arrived(3)
    across = [
        (from_next if s % 2 else from_prev)[s // 2 * width : (s // 2 + 1) * width]
        for s in range(subs)
    ]
    put(swapped_basis, (2,), jnp.concatenate(across, axis=0))
    id_rows = [id_row.astype(jnp.float32)]
    for i in (1, 0, 3, 2):
        first = coefs if i < 2 else coefs // 2
        id_rows.append(tables.slots[i][first : first + 1])
    picks = jnp.concatenate([hot_of(row) for row in id_rows], axis=1).astype(jnp.bfloat16)
    for r in range(0, order, 2 * LANES):
        chunk = slice(r, min(r + 2 * LANES, order))
        for i, half in enumerate(halves(global_ref[chunk])):
            picked_ref[i, chunk] = dot(half, picks, NN, None).astype(jnp.bfloat16)
    rhs_swapped = rhs_swap.field()
    odd = lax.rem(lane // width, 2) == 1
    cross_ids = jnp.where(odd, id_rows[3], id_rows[4])
    for i, row in enumerate((id_rows[1], id_rows[2], cross_ids)):
        put_hot(i + 1, row)

    coarse_run("wait_recv")
    for slot, has in enumerate((has_high, has_low)):
        put_solve((slot + 1) * coefs, jnp.where(has, near_coarse[slot], 0.0))

    fix, fix_swapped, row = correction(tail, [share])
    rho = as_column(row)
    direction = rhs - fix
    spread = sign * (direction + rhs_swapped - fix_swapped)
    image = image_of(spread.astype(jnp.bfloat16))
    signed = sign * image
    halved = stacked(signed)
    cross = swapped_raw(halved, 2)
    cross_refs[0][...] = cross
    pl.when(has_next)(lambda: cross_copy(0).start())
    pl.when(has_prev)(lambda: cross_copy(1).start())
    raw = [own_raw(halved), swapped_raw(halved, 0), swapped_raw(halved, 1), cross]
    tail, share, solve = sums(1, raw, dots(spread * image))
    tail.start()
    solve()
    share.start()
    swap = Swap(swap_refs, 0)
    swap.fill(signed, orders, loads)
    swap.start()
    pl.when(has_prev)(lambda: cross_copy(0).wait_recv())
    pl.when(has_next)(lambda: cross_copy(1).wait_recv())
    from_prev = jnp.where(has_prev, cross_refs[1][0], 0.0)
    from_next = jnp.where(has_next, cross_refs[1][1], 0.0)
    share_out(2, jnp.where(odd, from_prev, from_next))
    late = Shares(2)
    late.start()
    direction_swapped = rhs_swapped - fix_swapped
    signed_swapped = swap.field()
    product = signed + signed_swapped
    product_swapped = signed_swapped + there * signed

    fix, fix_swapped, row = correction(tail, [share, late])
    curvature = as_column(row)
    step = rho / curvature
    moved = direction - step * (product - fix)
    moved_swapped = direction_swapped - step * (product_swapped - fix_swapped)
    residual = rhs - step * product
    spread_moved = sign * (moved + moved_swapped)
    image_moved = image_of(stacked(spread_moved)[0])
    curve_refs[0][0] = dots(
        residual * residual,
        spread_moved * image_moved,
        spread_moved * image + spread * image_moved,
    )
    curve = AllSum(sizes, curve_refs, 0)
    curve.start()
    signed = sign * image_moved
    last_swap = Swap(swap_refs, 1)
    last_swap.fill(signed, orders, loads)
    last_swap.start()
    product_moved = signed + last_swap.field()
    row = curve.finish()
    open_sends.extend([swap, curve, last_swap])
    ratio = as_column(row) / rho
    last_curvature = as_column(row, loads) + ratio * (
        as_column(row, 2 * loads) + ratio * curvature
    )
    last_step = ratio * rho / last_curvature
    multipliers = (step + last_step * ratio) * direction + last_step * moved
    residual = residual - last_step * (product_moved + ratio * product)
    for s in range(subs):
        out_ref[0, s] = multipliers[s * loads : (s + 1) * loads]
        out_ref[1, s] = residual[s * loads : (s + 1) * loads]
    for spread in open_sends:
        spread.wait_send()
    each(members - 1, lambda k: gather_copy(k).wait_send())
    coarse_run("wait_send")
    pl.when(has_next)(lambda: cross_copy(0).wait_send())
    pl.when(has_prev)(lambda: cross_copy(1).wait_send())


def split(both_ref, mult_ref, res_ref, sems):
    copies = [
        pltpu.make_async_copy(both_ref.at[i], out, sems.at[i])
        for i, out in enumerate((mult_ref, res_ref))
    ]
    for copy in copies:
        copy.start()
    for copy in copies:
        copy.wait()


def local(sizes, *args):
    args = list(args)
    args[3] = jnp.transpose(args[3], (1, 0, 2))
    rhs, operators, signs, links, cluster_basis, corner_basis, ids, coarse, glob = args
    clusters, members = sizes
    subs, loads, dual = rhs.shape
    coefs = subs * (cluster_basis.shape[1] + corner_basis.shape[1])
    depth, order = glob.shape
    f32 = jnp.float32
    dma = pltpu.SemaphoreType.DMA

    def exchange(lead, block, receive):
        return [
            pltpu.VMEM(lead[:1] + block, f32),
            pltpu.VMEM(lead + receive, f32),
            dma(lead),
            dma(lead),
        ]

    def swap_scratch(count, height, extra):
        scratch = []
        for rows in (subs * height + extra, subs * height // 2 + extra):
            scratch += [
                pltpu.VMEM((count, 2, rows, LANES), f32),
                pltpu.VMEM((count, 2, rows, LANES), f32),
                dma((count, 2)),
                dma((count, 2)),
            ]
        return scratch

    def sum_scratch(count, block):
        scratch = []
        for axes in stages(sizes):
            scratch += exchange((count, peers_of(sizes, axes)), block, block)
        return scratch

    vmem = pl.BlockSpec(memory_space=pltpu.VMEM)
    scratch = [pltpu.VMEM(a.shape, a.dtype) for a in args]
    scratch[6] = pltpu.SMEM(ids.shape, ids.dtype)
    bf16 = jnp.bfloat16
    solved = members * coefs
    inside, columns = coarse.shape[1:]
    scratch += [
        dma((len(args),)),
        pltpu.VMEM((coefs, dual), f32),
        pltpu.VMEM((2, coefs, dual), bf16),
        pltpu.VMEM((2, 3, coefs, LANES), bf16),
        pltpu.VMEM((2, 3 * coefs, solved), bf16),
        pltpu.VMEM((4 * coefs, order), bf16),
        pltpu.VMEM((order, order), f32),
        pltpu.VMEM((2, order, 5 * coefs), bf16),
        dma((members - 1,)),
        dma((members - 1,)),
        pltpu.VMEM((2, inside, columns), f32),
        dma((2,)),
        dma((2,)),
        pltpu.VMEM((loads, coefs), f32),
        pltpu.VMEM((2, loads, coefs), f32),
        dma((2,)),
        dma((2,)),
        pltpu.VMEM((ITERS + 1, members, loads, coefs), f32),
    ]
    block, near = (loads, coefs), (min(3, members), loads, coefs)
    for lead, shape in (
        ((ITERS + 1, members), near),
        ((ITERS + 1, 2, members), block),
    ):
        scratch += [pltpu.VMEM(lead + shape, f32), dma(lead), dma(lead)]
    scratch += sum_scratch(ITERS, (loads + 1, order)) + sum_scratch(1, (1, LANES))
    scratch += swap_scratch(ITERS + 1, loads, 0)
    scratch += swap_scratch(1, coefs // subs, 8)
    both = pl.pallas_call(
        functools.partial(kernel, sizes),
        out_shape=pltpu.VMEM((2,) + rhs.shape, f32),
        in_specs=[pl.BlockSpec(memory_space=pltpu.HBM)] * len(args),
        out_specs=vmem,
        scratch_shapes=scratch,
        compiler_params=pltpu.CompilerParams(
            collective_id=0, has_side_effects=True, vmem_limit_bytes=56 << 20
        ),
    )(*args)
    return pl.pallas_call(
        split,
        out_shape=[jax.ShapeDtypeStruct(rhs.shape, f32)] * 2,
        in_specs=[vmem],
        out_specs=[pl.BlockSpec(memory_space=pltpu.HBM)] * 2,
        scratch_shapes=[dma((2,))],
        compiler_params=pltpu.CompilerParams(vmem_limit_bytes=4 << 20),
    )(both)


def solution(mesh):
    placed = (
        P(("cluster", "sub"), None, None),
        P(("cluster", "sub"), None, None),
        P(("cluster", "sub"), None),
        P(("cluster", "sub"), None, None),
        P(("cluster", "sub"), None, None),
        P(("cluster", "sub"), None, None),
        P(("cluster", "sub"), None),
        P("cluster", "sub", None),
        P("sub", None),
    )
    return jax.shard_map(
        functools.partial(local, (mesh.shape["cluster"], mesh.shape["sub"])),
        mesh=mesh,
        in_specs=placed,
        out_specs=(P(("cluster", "sub"), None, None), P(("cluster", "sub"), None, None)),
        check_vma=False,
    )
```

```python
import functools

import jax
import jax.numpy as jnp
from jax import lax
from jax.experimental import pallas as pl
from jax.experimental.pallas import tpu as pltpu
from jax.sharding import PartitionSpec as P

ITERS = 2
LANES = 128
UNROLL = 32
MESH = pl.DeviceIdType.MESH
HIGHEST = lax.Precision.HIGHEST
NN = (((1,), (0,)), ((), ()))
NT = (((1,), (1,)), ((), ()))


def dot(a, b, dims=NN, precision=HIGHEST):
    return lax.dot_general(a, b, dims, precision=precision, preferred_element_type=jnp.float32)


def halves(x):
    high = x.astype(jnp.bfloat16)
    return high, (x - high.astype(jnp.float32)).astype(jnp.bfloat16)


def stacked(a):
    high = a.astype(jnp.bfloat16).astype(jnp.float32)
    return jnp.concatenate([high, a - high], axis=0).astype(jnp.bfloat16), high.astype(jnp.bfloat16)


def dot2(a, b, dims=NN):
    rows = a.shape[0]
    out = dot(stacked(a)[0], b, dims, None)
    return out[:rows] + out[rows:]


def dot3(a, b, dims=NN):
    rows = a.shape[0]
    both, high = stacked(a)
    out = dot(both, b[0], dims, None)
    return out[:rows] + out[rows:] + dot(high, b[1], dims, None)


def put(ref, index, x):
    for i, half in enumerate(halves(x)):
        ref[(i,) + index] = half


def iota(shape, dim):
    return lax.broadcasted_iota(jnp.int32, shape, dim)


def each(count, body):
    if count <= UNROLL:
        for k in range(count):
            body(k)
    else:
        lax.fori_loop(0, count, lambda k, carry: (body(k), carry)[1], 0)


def total(ref, count, start):
    if count <= UNROLL:
        terms = [start] + [ref[k] for k in range(count)]
        while len(terms) > 1:
            terms = [sum(terms[i : i + 2][1:], terms[i]) for i in range(0, len(terms), 2)]
        return terms[0]
    return lax.fori_loop(0, count, lambda k, acc: acc + ref[k], start)


class Spread:
    def __init__(self, sizes, axes, source, slots, send, recv):
        self.sizes, self.axes = sizes, axes
        self.source, self.slots, self.send, self.recv = source, slots, send, recv
        self.count = peers_of(sizes, axes)

    def copy(self, k):
        return pltpu.make_async_remote_copy(
            src_ref=self.source,
            dst_ref=self.slots.at[k],
            send_sem=self.send.at[k],
            recv_sem=self.recv.at[k],
            device_id=peer(self.sizes, self.axes, k),
            device_id_type=MESH,
        )

    def start(self):
        each(self.count, lambda k: self.copy(k).start())

    def wait_recv(self):
        each(self.count, lambda k: self.copy(k).wait_recv())

    def wait_send(self):
        each(self.count, lambda k: self.copy(k).wait_send())


def peers_of(sizes, axes):
    clusters, members = sizes
    return {"both": clusters * members, "cluster": clusters, "sub": members}[axes] - 1


def peer(sizes, axes, k):
    clusters, members = sizes
    if axes == "both":
        c, m = (k + 1) // members, (k + 1) % members
        return {
            "cluster": lax.rem(lax.axis_index("cluster") + c, clusters),
            "sub": lax.rem(lax.axis_index("sub") + m, members),
        }
    count = clusters if axes == "cluster" else members
    return {axes: lax.rem(lax.axis_index(axes) + k + 1, count)}


def stages(sizes):
    return ("both",) if sizes[0] * sizes[1] <= UNROLL else ("cluster", "sub")


class AllSum:
    def __init__(self, sizes, refs, n):
        self.spreads = []
        for i, axes in enumerate(stages(sizes)):
            source, slots, send, recv = refs[4 * i : 4 * i + 4]
            self.spreads.append(
                Spread(sizes, axes, source.at[n], slots.at[n], send.at[n], recv.at[n])
            )

    def start(self):
        self.spreads[0].start()

    def finish(self):
        for i, spread in enumerate(self.spreads):
            spread.wait_recv()
            out = total(spread.slots, spread.count, spread.source[...])
            if i + 1 < len(self.spreads):
                self.spreads[i + 1].source[...] = out
                self.spreads[i + 1].start()
        return out

    def wait_send(self):
        for spread in self.spreads:
            spread.wait_send()


def kernel(sizes, *refs):
    clusters, members = sizes
    hbm, out_ref, refs = refs[:9], refs[9], list(refs[10:])

    def take_refs(count):
        taken = refs[:count]
        del refs[:count]
        return taken

    local_refs = take_refs(9)
    (
        rhs_ref,
        ops_ref,
        signs_ref,
        links_ref,
        cluster_basis_ref,
        corner_basis_ref,
        ids_ref,
        cluster_coarse_ref,
        global_coarse_ref,
    ) = local_refs
    (local_sem,) = take_refs(1)
    basis_ref, basis_halves, swapped_basis, solve_ref, hot_ref = take_refs(5)
    global_ref, picked_ref = take_refs(2)
    g_send, g_recv = take_refs(2)
    near_coarse, near_send, near_recv = take_refs(3)
    cross_refs = take_refs(4)
    cross_map, cross_image = take_refs(2)
    (share_ref,) = take_refs(1)
    share_refs = [take_refs(3) for _ in range(2)]
    sum_refs = [take_refs(4 * len(stages(sizes))) for _ in range(ITERS)]
    curve_refs = take_refs(4 * len(stages(sizes)))
    swap_refs = take_refs(8)
    table_refs = take_refs(8)

    subs, loads, dual = rhs_ref.shape
    rows = subs * loads
    kc, corn = cluster_basis_ref.shape[1], corner_basis_ref.shape[1]
    width = kc + corn
    coefs = subs * width
    order = global_coarse_ref.shape[1]
    solved = members * coefs
    near = share_refs[0][0].shape[2]
    my_c, my_s = lax.axis_index("cluster"), lax.axis_index("sub")
    has_low, has_high = my_s > 0, my_s < members - 1
    has_prev, has_next = my_c > 0, my_c < clusters - 1

    def run(copies, what, there=None):
        def act():
            for copy in copies:
                getattr(copy, what)()

        act() if there is None else pl.when(there)(act)


    barrier = pltpu.get_barrier_semaphore()

    def greet(device_id):
        pl.semaphore_signal(barrier, inc=1, device_id=device_id, device_id_type=MESH)

    greeted = 0
    for axes in ("both",) if len(stages(sizes)) == 1 else ("cluster", "sub"):
        count = peers_of(sizes, axes)
        each(count, lambda k, axes=axes: greet(peer(sizes, axes, k)))
        greeted += count
    if len(stages(sizes)) > 1:
        for there, step in ((has_next, 1), (has_prev, -1)):

            @pl.when(there)
            def _():
                for m in range(1, members):
                    greet({"cluster": my_c + step, "sub": lax.rem(my_s + m, members)})

            greeted = greeted + there.astype(jnp.int32) * (members - 1)

    loads_in = [
        pltpu.make_async_copy(hbm[i], local_refs[i], local_sem.at[i]) for i in range(len(hbm))
    ]
    for i in (6, 5, 4, 0, 7, 8, 3, 2, 1):
        loads_in[i].start()
    numbers = iota((8, LANES), 1).astype(jnp.bfloat16)

    loads_in[6].wait()
    id_row = jnp.full((1, coefs), -1, jnp.int32)
    lane = iota((1, coefs), 1)
    for s in range(subs):
        for c in range(corn):
            id_row = jnp.where(lane == s * width + kc + c, ids_ref[s, c], id_row)
    whose = iota((order, coefs), 0).astype(jnp.float32)
    corner_of = iota((coefs, order), 1).astype(jnp.float32)

    def hot_of(row):
        return (row == whose).astype(jnp.float32)

    def put_hot(i, row):
        same = iota((coefs, coefs), 0) == iota((coefs, coefs), 1)
        column = jnp.sum(jnp.where(same, row, 0.0), axis=1, keepdims=True)
        hot = (column == corner_of).astype(jnp.float32)
        hot_ref[i * coefs : (i + 1) * coefs] = hot.astype(jnp.bfloat16)

    put_hot(0, id_row.astype(jnp.float32))

    loads_in[5].wait()
    loads_in[4].wait()
    for s in range(subs):
        basis_ref[s * width : s * width + kc, :] = cluster_basis_ref[s]
        basis_ref[s * width + kc : (s + 1) * width, :] = corner_basis_ref[s]
    put(basis_halves, (), basis_ref[...])

    where_to = iota((1, solved), 1)
    within = lax.rem(where_to, width)
    source = (where_to // coefs) * (subs * kc) + (lax.rem(where_to, coefs) // width) * kc + within
    source = jnp.where(within < kc, source, -1)
    place = (iota((members * subs * kc, solved), 0) == source).astype(jnp.float32)
    place = place.astype(jnp.bfloat16)

    def placed(x):
        return [dot(half, place, NN, None).astype(jnp.bfloat16) for half in halves(x)]

    solve_ref[...] = jnp.zeros(solve_ref.shape, jnp.bfloat16)

    def put_solve(first, x):
        for i, half in enumerate(placed(x)):
            for s in range(subs):
                at = first + s * width
                solve_ref[i, at : at + kc] = half[s * kc : (s + 1) * kc]

    loads_in[0].wait()
    loads_in[7].wait()
    put_solve(0, cluster_coarse_ref[0])

    diagonal = iota((rows, coefs), 0) // loads == iota((rows, coefs), 1) // width
    row_sub, lane_sub = iota((rows, coefs), 0) // loads, iota((rows, coefs), 1) // width
    crossed = row_sub + 1 - 2 * lax.rem(row_sub, 2) == lane_sub
    inner, outer = slice(0, 2 * LANES), slice(2 * LANES, dual)

    def per_load(x):
        out = x[:loads]
        for s in range(1, subs):
            out = out + x[s * loads : (s + 1) * loads]
        return out

    def lanes_added(x):
        out = x[:, :LANES]
        for b in range(1, dual // LANES):
            out = out + x[:, b * LANES : (b + 1) * LANES]
        return out

    def tiled(x):
        return jnp.concatenate([x] * subs, axis=0)

    def as_row(x):
        shape = (x.shape[0], LANES)
        sums = jnp.sum(x, axis=1, keepdims=True)
        kept = jnp.where(iota(shape, 0) == iota(shape, 1), sums, 0.0)
        return jnp.sum(kept, axis=0, keepdims=True)

    def as_column(x, first=0):
        mine = iota((rows, LANES), 1) == lax.rem(iota((rows, LANES), 0), loads) + first
        return jnp.sum(jnp.where(mine, x, 0.0), axis=1, keepdims=True)

    def dots(*products):
        return as_row(jnp.concatenate([per_load(lanes_added(x)) for x in products], axis=0))

    open_sends = []

    def first_near(member):
        return jnp.clip(member - 1, 0, members - near)

    def near_part(ref, target):
        return ref.at[pl.ds(first_near(target), near)]

    def push(refs, at, source, step, target):
        slots, send, recv = refs
        device_id = {"sub": target}
        if step:
            device_id["cluster"] = my_c + step
        return pltpu.make_async_remote_copy(
            src_ref=source,
            dst_ref=slots.at[at],
            send_sem=send.at[at],
            recv_sem=recv.at[at],
            device_id=device_id,
            device_id_type=MESH,
        )

    class Shares:
        def __init__(self, n):
            own, pieces = share_refs
            self.n = n
            mine = share_ref.at[n]

            def target(k):
                return lax.rem(my_s + k, members)

            def copies(refs, lead, of, step, ks):
                return [push(refs, lead + (k,), of(target(k)), step, target(k)) for k in ks]

            near_mine = functools.partial(near_part, mine)
            self.near = copies(own, (n,), near_mine, 0, range(1, members))
            self.sides = [
                copies(pieces, (n, side), lambda t: mine.at[t], 1 - 2 * side, range(members))
                for side in range(2)
            ]

        def start(self):
            self.run_sides("start", has_next, has_prev)
            run(self.near, "start")

        def wait_send(self):
            self.run_sides("wait_send", has_next, has_prev)
            run(self.near, "wait_send")

        def run_sides(self, what, *theres):
            for copies, there in zip(self.sides, theres):
                run(copies, what, there)

        def sum_of(self, terms):
            while len(terms) > 1:
                terms = [sum(terms[i : i + 2][1:], terms[i]) for i in range(0, len(terms), 2)]
            return terms[0]

        def of_near(self):
            for copy in self.near:
                copy.wait_recv()
            slots, base = share_refs[0][0], first_near(my_s)

            def of_member(member):
                near_slots = [slots[self.n, k, member - base] for k in range(1, members)]
                return self.sum_of([share_ref[self.n, member]] + near_slots)

            high = of_member(jnp.minimum(my_s + 1, members - 1))
            low = of_member(jnp.maximum(my_s - 1, 0))
            return of_member(my_s), high, low

        def of_sides(self):
            self.run_sides("wait_recv", has_prev, has_next)
            slots = share_refs[1][0]
            prev, following = [
                self.sum_of([slots[self.n, side, k] for k in range(members)]) for side in range(2)
            ]
            odd = lax.rem(iota((loads, coefs), 1) // width, 2) == 1
            following = jnp.where(has_next, following, 0.0)
            return jnp.where(odd, following, jnp.where(has_prev, prev, 0.0))

    def sums(n, raw, row):
        tail_refs = sum_refs[n]
        tail_refs[0][0, :loads] = dot2(
            jnp.concatenate(raw, axis=1), hot_ref[: len(raw) * coefs]
        )
        if row is not None:
            tail_refs[0][0, loads:, :LANES] = row
            if order > LANES:
                tail_refs[0][0, loads:, LANES:] = jnp.zeros((1, order - LANES), jnp.float32)
        tail = AllSum(sizes, tail_refs, 0)
        share = Shares(n)

        def solve():
            share_out(n, jnp.concatenate(raw[:3], axis=1))

        return tail, share, solve

    def share_out(n, inside):
        out = dot3(inside, [solve_ref[i, : inside.shape[1]] for i in range(2)])
        for j in range(members):
            share_ref[n, j] = out[:, j * coefs : (j + 1) * coefs]

    def block_diagonal(x, mask):
        return jnp.where(mask, tiled(x), 0.0)

    def raw_of(halved, lanes, b, mask):
        both, high = halved
        out = dot(both[:, lanes], b[0], NT, None)
        x = out[:rows] + out[rows:] + dot(high[:, lanes], b[1], NT, None)
        return per_load(jnp.where(mask, x, 0.0))

    def own_raw(halved):
        return raw_of(halved, slice(0, dual), basis_halves, diagonal)

    def swapped_raw(halved, i, lanes):
        b = [swapped_basis[0, i], swapped_basis[1, i]]
        return raw_of(halved, lanes, b, crossed if i == 2 else diagonal)

    def correction(tail, share, late=None, between=lambda: None):
        own, high, low = share.of_near()
        cross = share.of_sides()
        summed = tail.finish()
        out = dot3(summed[:loads], picked_ref)
        between()
        near = [x + out[:, i * coefs : (i + 1) * coefs] for i, x in enumerate((own, high, low))]
        open_sends.extend([tail, share])
        if late is not None:
            near = [x + more for x, more in zip(near, late.of_near())]
            open_sends.append(late)
        masked = [block_diagonal(x, diagonal) for x in near]
        fix = dot3(masked[0], basis_halves)
        swapped = [
            dot3(masked[i + 1], [swapped_basis[0, i], swapped_basis[1, i]]) for i in range(2)
        ]

        def last():
            total = cross + out[:, 3 * coefs :]
            if late is not None:
                total = total + late.of_sides()
            masked = block_diagonal(total, crossed)
            return dot3(masked, [swapped_basis[0, 2], swapped_basis[1, 2]]), masked

        return fix, jnp.concatenate(swapped, axis=1), last, summed[loads:, :LANES]

    def image_of(spread, depth, columns):
        out = None
        for s in range(subs):
            x = dot(spread, ops_ref[s, depth, columns], NN, None)
            if x.shape[0] > rows:
                x = x[:rows] + x[rows:]
            out = x if out is None else jnp.where(iota(x.shape, 0) // loads == s, x, out)
        return out

    def take(x, order_of):
        return jnp.take_along_axis(x, order_of, axis=1, mode="promise_in_bounds")

    class Swap:
        def __init__(self, refs, n):
            in_src, in_slots, in_send, in_recv, out_src, out_slots, out_send, out_recv = refs
            self.sources = [in_src.at[n, 0], in_src.at[n, 1], out_src.at[n, 0], out_src.at[n, 1]]
            self.slots = [
                in_slots.at[n, 0],
                in_slots.at[n, 1],
                out_slots.at[n, 0],
                out_slots.at[n, 1],
            ]
            self.send = [in_send.at[n, 0], in_send.at[n, 1], out_send.at[n, 0], out_send.at[n, 1]]
            self.recv = [in_recv.at[n, 0], in_recv.at[n, 1], out_recv.at[n, 0], out_recv.at[n, 1]]
            self.sends = [has_high, has_low, has_next, has_prev]
            self.takes = [has_low, has_high, has_prev, has_next]

        def copy(self, i):
            axis = "sub" if i < 2 else "cluster"
            return pltpu.make_async_remote_copy(
                src_ref=self.sources[i],
                dst_ref=self.slots[i],
                send_sem=self.send[i],
                recv_sem=self.recv[i],
                device_id={axis: lax.axis_index(axis) + (-1 if i % 2 else 1)},
                device_id_type=MESH,
            )

        def fill(self, x, orders, height, extra=None):
            up_order, down_order, across_order = orders
            count = subs * height
            across = take(x[:, 2 * LANES :], across_order)
            for p in range(2):
                for h in range(subs // 2):
                    s = 2 * h + p
                    self.sources[2 + p][h * height : (h + 1) * height] = across[
                        s * height : (s + 1) * height
                    ]
            self.sources[0][:count] = take(x[:, :LANES], up_order)
            self.sources[1][:count] = take(x[:, LANES : 2 * LANES], down_order)
            if extra is not None:
                for i in range(4):
                    first = count if i < 2 else count // 2
                    self.sources[i][first : first + 8] = extra

        def start(self):
            for i in (2, 3, 0, 1):
                pl.when(self.sends[i])(self.copy(i).start)

        def wait_recv(self, which=range(4)):
            for i in which:
                pl.when(self.takes[i])(self.copy(i).wait_recv)

        def wait_send(self):
            for i in range(4):
                pl.when(self.sends[i])(self.copy(i).wait_send)

        def arrived(self, i):
            return jnp.where(self.takes[i], self.slots[i][...], 0.0)

        def field(self):
            at_odd, at_even = self.arrived(2), self.arrived(3)
            across = [
                (at_odd if s % 2 else at_even)[s // 2 * loads : (s // 2 + 1) * loads]
                for s in range(subs)
            ]
            return jnp.concatenate(
                [self.arrived(1), self.arrived(0), jnp.concatenate(across, axis=0)], axis=1
            )

    depth = global_coarse_ref.shape[0]
    own_rows = pl.ds(pl.multiple_of(my_s * depth, 8), depth)

    def gather_copy(k):
        return pltpu.make_async_remote_copy(
            src_ref=global_coarse_ref,
            dst_ref=global_ref.at[own_rows],
            send_sem=g_send.at[k],
            recv_sem=g_recv.at[k],
            device_id=peer(sizes, "sub", k),
            device_id_type=MESH,
        )

    def near_copy(slot):
        return pltpu.make_async_remote_copy(
            src_ref=cluster_coarse_ref.at[0],
            dst_ref=near_coarse.at[slot],
            send_sem=near_send.at[slot],
            recv_sem=near_recv.at[slot],
            device_id={"sub": my_s + (1 if slot else -1)},
            device_id_type=MESH,
        )

    def cross_copy(slot):
        there, step = (has_prev, -1) if slot else (has_next, 1)
        lands = jnp.where(there, slot, slot + 2)
        return pltpu.make_async_remote_copy(
            src_ref=cross_refs[0],
            dst_ref=cross_refs[1].at[lands],
            send_sem=cross_refs[2].at[slot],
            recv_sem=cross_refs[3].at[lands],
            device_id={"cluster": my_c + jnp.where(there, step, -step)},
            device_id_type=MESH,
        )

    def cross_wait(slot, there):
        copy = pltpu.make_async_remote_copy(
            src_ref=cross_refs[0],
            dst_ref=cross_refs[1].at[slot],
            send_sem=cross_refs[2].at[slot % 2],
            recv_sem=cross_refs[3].at[slot],
            device_id={"cluster": my_c},
            device_id_type=MESH,
        )
        pl.when(there)(copy.wait_recv)

    coarse_copies = [near_copy(0), near_copy(1)]
    cross_copies = [cross_copy(0), cross_copy(1)]

    def plain(row):
        return row

    def inverted(row):
        hot = (iota((LANES, LANES), 0) == row).astype(jnp.float32).astype(jnp.bfloat16)
        return dot(numbers, hot, NT, None)[:1].astype(jnp.int32)

    loads_in[3].wait()
    index = [
        [inverted(links_ref[0, s : s + 1, :]) for s in range(subs)],
        [plain(links_ref[1, s : s + 1, :]) for s in range(subs)],
        [(plain if s % 2 else inverted)(links_ref[2, s : s + 1, :]) for s in range(subs)],
    ]

    def orders_of(height):
        return [
            jnp.concatenate([jnp.broadcast_to(row, (height, LANES)) for row in block], axis=0)
            for block in index
        ]

    rhs = jnp.concatenate([rhs_ref[s] for s in range(subs)], axis=0)
    orders = orders_of(loads)
    rhs_swap, tables = Swap(swap_refs, ITERS), Swap(table_refs, 0)
    rhs_swap.fill(rhs, orders, loads)
    ids_sent = jnp.broadcast_to(id_row.astype(jnp.float32), (8, coefs))
    tables.fill(basis_ref[...], orders_of(width), width, ids_sent)
    tail, share, solve = sums(0, [own_raw(stacked(rhs))], None)
    solve()
    loads_in[8].wait()
    global_ref[own_rows, :] = global_coarse_ref[...]
    pl.semaphore_wait(barrier, greeted)
    tail.start()
    share.start()
    tables.start()
    each(members - 1, lambda k: gather_copy(k).start())
    rhs_swap.start()
    run(coarse_copies[:1], "start", has_low)
    run(coarse_copies[1:], "start", has_high)

    loads_in[2].wait()
    sign = jnp.concatenate(
        [
            jnp.broadcast_to(signs_ref[s : s + 1, :].astype(jnp.float32), (loads, dual))
            for s in range(subs)
        ],
        axis=0,
    )
    row_odd = lax.rem(iota((rows, LANES), 0) // loads, 2) == 1
    there = jnp.concatenate(
        [
            jnp.full((rows, LANES), has_high.astype(jnp.float32)),
            jnp.full((rows, LANES), has_low.astype(jnp.float32)),
            jnp.where(row_odd, has_prev.astype(jnp.float32), has_next.astype(jnp.float32)),
        ],
        axis=1,
    )
    loads_in[1].wait()
    open_sends.extend([rhs_swap, tables])
    each(members - 1, lambda k: gather_copy(k).wait_recv())
    partner = [s + 1 - 2 * (s % 2) for s in range(subs)]
    own_ids = id_row.astype(jnp.float32)

    def pick(first, id_rows):
        picks = jnp.concatenate([hot_of(row) for row in id_rows], axis=1).astype(jnp.bfloat16)
        lanes = slice(first * coefs, (first + len(id_rows)) * coefs)
        for r in range(0, order, 2 * LANES):
            chunk = slice(r, min(r + 2 * LANES, order))
            for i, half in enumerate(halves(global_ref[chunk])):
                picked_ref[i, chunk, lanes] = dot(half, picks, NN, None).astype(jnp.bfloat16)

    tables.wait_recv(range(2))
    put(swapped_basis, (0,), tables.arrived(1)[:coefs])
    put(swapped_basis, (1,), tables.arrived(0)[:coefs])
    id_rows = [own_ids] + [tables.slots[i][coefs : coefs + 1] for i in (1, 0)]
    pick(0, id_rows)
    for i in range(1, 3):
        put_hot(i, id_rows[i])
    rhs_swap.wait_recv(range(2))
    tables.wait_recv(range(2, 4))
    from_prev, from_next = tables.arrived(2), tables.arrived(3)
    across = [
        (from_next if s % 2 else from_prev)[s // 2 * width : (s // 2 + 1) * width]
        for s in range(subs)
    ]
    across = jnp.concatenate(across, axis=0)
    put(swapped_basis, (2,), across)
    odd = lax.rem(lane // width, 2) == 1
    cross_ids = [tables.slots[i][coefs // 2 : coefs // 2 + 1] for i in (3, 2)]
    cross_ids = jnp.where(odd, *cross_ids)
    pick(3, [cross_ids])
    across = across * jnp.concatenate(
        [
            jnp.broadcast_to(sign[loads * s : loads * s + 1, outer], (width, LANES))
            for s in partner
        ],
        axis=0,
    )
    rhs_swap.wait_recv(range(2, 4))
    rhs_swapped = rhs_swap.field()

    def map_cross():
        across_halves = jnp.concatenate(halves(across), axis=1)
        out = None
        for s in range(subs):
            twice = jnp.concatenate([ops_ref[s, :, outer]] * 2, axis=1)
            x = dot(twice, across_halves, NT, None)
            out = x if out is None else jnp.where(iota(x.shape, 1) // width == partner[s], x, out)
        for i, half in enumerate(halves(out)):
            cross_map[:, i * coefs : (i + 1) * coefs] = half
        put_hot(3, cross_ids)

    fix, fix_swapped, last, _ = correction(tail, share, between=map_cross)
    fix_swapped = jnp.concatenate([fix_swapped, last()[0]], axis=1)
    direction = rhs - fix
    direction_swapped = rhs_swapped - fix_swapped
    spread = sign * (direction + direction_swapped)
    spread_bf = spread.astype(jnp.bfloat16)
    everything = slice(0, dual)
    out = dot(spread_bf, cross_map[...], NN, None)
    out = out[:, :coefs] + out[:, coefs:]
    cross = per_load(jnp.where(crossed, out, 0.0))
    image = image_of(spread_bf, everything, everything)
    cross_refs[0][...] = cross
    run(cross_copies, "start")
    signed = sign * image
    halved = stacked(signed)
    raw = [own_raw(halved)]
    raw += [swapped_raw(halved, i, slice(i * LANES, (i + 1) * LANES)) for i in range(2)]
    raw.append(cross)
    tail, share, solve = sums(1, raw, dots(spread * image, rhs * rhs))
    tail.start()
    run(coarse_copies[:1], "wait_recv", has_high)
    run(coarse_copies[1:], "wait_recv", has_low)
    for slot, has in enumerate((has_high, has_low)):
        put_solve((slot + 1) * coefs, jnp.where(has, near_coarse[slot], 0.0))
    solve()
    share.start()
    for s in range(subs):
        mine = slice(partner[s] * width, (partner[s] + 1) * width)
        x = dot(stacked(across[mine])[0], ops_ref[s, outer, :], NN, None)
        put(cross_image, (mine,), x[:width] + x[width:])
    swap = Swap(swap_refs, 0)
    swap.fill(signed, orders, loads)
    swap.start()
    cross_wait(0, has_prev)
    cross_wait(1, has_next)
    from_prev = jnp.where(has_prev, cross_refs[1][0], 0.0)
    from_next = jnp.where(has_next, cross_refs[1][1], 0.0)
    share_out(2, jnp.where(odd, from_prev, from_next))
    late = Shares(2)
    late.start()
    swap.wait_recv()
    signed_swapped = swap.field()
    product = signed + signed_swapped
    product_swapped = signed_swapped + there * signed

    fix, fix_swapped, last, row = correction(tail, share, late)
    curvature, rho = as_column(row), as_column(row, loads)
    step = rho / curvature
    residual = rhs - step * product
    moved = direction - step * (product - fix)

    fix_swapped = jnp.concatenate([fix_swapped, jnp.zeros((rows, LANES), jnp.float32)], axis=1)
    moved_swapped = direction_swapped - step * (product_swapped - fix_swapped)
    spread_moved = sign * (moved + moved_swapped)
    image_moved = image_of(stacked(spread_moved)[0], everything, everything)
    last_fix, masked = last()
    image_moved = image_moved + step * dot3(masked, cross_image)
    last_fix = step * sign[:, outer] * last_fix
    spread_moved = jnp.concatenate(
        [spread_moved[:, inner], spread_moved[:, outer] + last_fix], axis=1
    )
    curve_refs[0][0] = dots(
        residual * residual,
        spread_moved * image_moved,
        spread_moved * image + spread * image_moved,
    )
    curve = AllSum(sizes, curve_refs, 0)
    curve.start()
    signed = sign * image_moved
    last_swap = Swap(swap_refs, 1)
    last_swap.fill(signed, orders, loads)
    last_swap.start()
    last_swap.wait_recv()
    product_moved = signed + last_swap.field()
    for spread in open_sends + [swap]:
        spread.wait_send()
    each(members - 1, lambda k: gather_copy(k).wait_send())
    run(coarse_copies[:1], "wait_send", has_low)
    run(coarse_copies[1:], "wait_send", has_high)
    run(cross_copies, "wait_send")
    cross_wait(2, my_c == clusters - 2)
    cross_wait(3, my_c == 1)
    row = curve.finish()
    ratio = as_column(row) / rho
    last_curvature = as_column(row, loads) + ratio * (
        as_column(row, 2 * loads) + ratio * curvature
    )
    last_step = ratio * rho / last_curvature
    multipliers = (step + last_step * ratio) * direction + last_step * moved
    residual = residual - last_step * (product_moved + ratio * product)
    for s in range(subs):
        out_ref[0, s] = multipliers[s * loads : (s + 1) * loads]
        out_ref[1, s] = residual[s * loads : (s + 1) * loads]
    curve.wait_send()
    last_swap.wait_send()


def split(both_ref, mult_ref, res_ref, sems):
    copies = [
        pltpu.make_async_copy(both_ref.at[i], out, sems.at[i])
        for i, out in enumerate((mult_ref, res_ref))
    ]
    for copy in copies:
        copy.start()
    for copy in copies:
        copy.wait()


def local(sizes, *args):
    args = list(args)
    args[3] = jnp.transpose(args[3], (1, 0, 2))
    rhs, operators, signs, links, cluster_basis, corner_basis, ids, coarse, glob = args
    clusters, members = sizes
    subs, loads, dual = rhs.shape
    coefs = subs * (cluster_basis.shape[1] + corner_basis.shape[1])
    depth, order = glob.shape
    f32 = jnp.float32
    dma = pltpu.SemaphoreType.DMA

    def exchange(lead, block, receive):
        return [
            pltpu.VMEM(lead[:1] + block, f32),
            pltpu.VMEM(lead + receive, f32),
            dma(lead),
            dma(lead),
        ]

    def swap_scratch(count, height, extra):
        scratch = []
        for rows in (subs * height + extra, subs * height // 2 + extra):
            scratch += [
                pltpu.VMEM((count, 2, rows, LANES), f32),
                pltpu.VMEM((count, 2, rows, LANES), f32),
                dma((count, 2)),
                dma((count, 2)),
            ]
        return scratch

    def sum_scratch(count, block):
        scratch = []
        for axes in stages(sizes):
            scratch += exchange((count, peers_of(sizes, axes)), block, block)
        return scratch

    vmem = pl.BlockSpec(memory_space=pltpu.VMEM)
    scratch = [pltpu.VMEM(a.shape, a.dtype) for a in args]
    scratch[6] = pltpu.SMEM(ids.shape, ids.dtype)
    bf16 = jnp.bfloat16
    solved = members * coefs
    inside, columns = coarse.shape[1:]
    scratch += [
        dma((len(args),)),
        pltpu.VMEM((coefs, dual), f32),
        pltpu.VMEM((2, coefs, dual), bf16),
        pltpu.VMEM((2, 3, coefs, LANES), bf16),
        pltpu.VMEM((2, 3 * coefs, solved), bf16),
        pltpu.VMEM((4 * coefs, order), bf16),
        pltpu.VMEM((order, order), f32),
        pltpu.VMEM((2, order, 4 * coefs), bf16),
        dma((members - 1,)),
        dma((members - 1,)),
        pltpu.VMEM((2, inside, columns), f32),
        dma((2,)),
        dma((2,)),
        pltpu.VMEM((loads, coefs), f32),
        pltpu.VMEM((4, loads, coefs), f32),
        dma((2,)),
        dma((4,)),
        pltpu.VMEM((dual, 2 * coefs), bf16),
        pltpu.VMEM((2, coefs, dual), bf16),
        pltpu.VMEM((ITERS + 1, members, loads, coefs), f32),
    ]
    block, near = (loads, coefs), (min(3, members), loads, coefs)
    for lead, shape in (
        ((ITERS + 1, members), near),
        ((ITERS + 1, 2, members), block),
    ):
        scratch += [pltpu.VMEM(lead + shape, f32), dma(lead), dma(lead)]
    scratch += sum_scratch(1, (loads, order)) + sum_scratch(1, (loads + 1, order))
    scratch += sum_scratch(1, (1, LANES))
    scratch += swap_scratch(ITERS + 1, loads, 0)
    scratch += swap_scratch(1, coefs // subs, 8)
    both = pl.pallas_call(
        functools.partial(kernel, sizes),
        out_shape=pltpu.VMEM((2,) + rhs.shape, f32),
        in_specs=[pl.BlockSpec(memory_space=pltpu.HBM)] * len(args),
        out_specs=vmem,
        scratch_shapes=scratch,
        compiler_params=pltpu.CompilerParams(
            collective_id=0, has_side_effects=True, vmem_limit_bytes=56 << 20
        ),
    )(*args)
    return pl.pallas_call(
        split,
        out_shape=[jax.ShapeDtypeStruct(rhs.shape, f32)] * 2,
        in_specs=[vmem],
        out_specs=[pl.BlockSpec(memory_space=pltpu.HBM)] * 2,
        scratch_shapes=[dma((2,))],
        compiler_params=pltpu.CompilerParams(vmem_limit_bytes=4 << 20),
    )(both)


def solution(mesh):
    placed = (
        P(("cluster", "sub"), None, None),
        P(("cluster", "sub"), None, None),
        P(("cluster", "sub"), None),
        P(("cluster", "sub"), None, None),
        P(("cluster", "sub"), None, None),
        P(("cluster", "sub"), None, None),
        P(("cluster", "sub"), None),
        P("cluster", "sub", None),
        P("sub", None),
    )
    return jax.shard_map(
        functools.partial(local, (mesh.shape["cluster"], mesh.shape["sub"])),
        mesh=mesh,
        in_specs=placed,
        out_specs=(P(("cluster", "sub"), None, None), P(("cluster", "sub"), None, None)),
        check_vma=False,
    )
```

```python
import functools

import jax
import jax.numpy as jnp
from jax import lax
from jax.experimental import pallas as pl
from jax.experimental.pallas import tpu as pltpu
from jax.sharding import PartitionSpec as P

ITERS = 2
LANES = 128
UNROLL = 32
MESH = pl.DeviceIdType.MESH
HIGHEST = lax.Precision.HIGHEST
NN = (((1,), (0,)), ((), ()))
NT = (((1,), (1,)), ((), ()))


def dot(a, b, dims=NN, precision=HIGHEST):
    return lax.dot_general(a, b, dims, precision=precision, preferred_element_type=jnp.float32)


def halves(x):
    high = x.astype(jnp.bfloat16)
    return high, (x - high.astype(jnp.float32)).astype(jnp.bfloat16)


def stacked(a):
    high = a.astype(jnp.bfloat16).astype(jnp.float32)
    return jnp.concatenate([high, a - high], axis=0).astype(jnp.bfloat16), high.astype(jnp.bfloat16)


def dot2(a, b, dims=NN):
    rows = a.shape[0]
    out = dot(stacked(a)[0], b, dims, None)
    return out[:rows] + out[rows:]


def dot3(a, b, dims=NN):
    rows = a.shape[0]
    both, high = stacked(a)
    out = dot(both, b[0], dims, None)
    return out[:rows] + out[rows:] + dot(high, b[1], dims, None)


def put(ref, index, x):
    for i, half in enumerate(halves(x)):
        ref[(i,) + index] = half


def iota(shape, dim):
    return lax.broadcasted_iota(jnp.int32, shape, dim)


def each(count, body):
    if count <= UNROLL:
        for k in range(count):
            body(k)
    else:
        lax.fori_loop(0, count, lambda k, carry: (body(k), carry)[1], 0)


def total(ref, count, start):
    if count <= UNROLL:
        terms = [start] + [ref[k] for k in range(count)]
        while len(terms) > 1:
            terms = [sum(terms[i : i + 2][1:], terms[i]) for i in range(0, len(terms), 2)]
        return terms[0]
    return lax.fori_loop(0, count, lambda k, acc: acc + ref[k], start)


class Spread:
    def __init__(self, sizes, axes, source, slots, send, recv):
        self.sizes, self.axes = sizes, axes
        self.source, self.slots, self.send, self.recv = source, slots, send, recv
        self.count = peers_of(sizes, axes)

    def copy(self, k):
        return pltpu.make_async_remote_copy(
            src_ref=self.source,
            dst_ref=self.slots.at[k],
            send_sem=self.send.at[k],
            recv_sem=self.recv.at[k],
            device_id=peer(self.sizes, self.axes, k),
            device_id_type=MESH,
        )

    def start(self):
        each(self.count, lambda k: self.copy(k).start())

    def wait_recv(self):
        each(self.count, lambda k: self.copy(k).wait_recv())

    def wait_send(self):
        each(self.count, lambda k: self.copy(k).wait_send())


def peers_of(sizes, axes):
    clusters, members = sizes
    return {"both": clusters * members, "cluster": clusters, "sub": members}[axes] - 1


def peer(sizes, axes, k):
    clusters, members = sizes
    if axes == "both":
        c, m = (k + 1) // members, (k + 1) % members
        return {
            "cluster": lax.rem(lax.axis_index("cluster") + c, clusters),
            "sub": lax.rem(lax.axis_index("sub") + m, members),
        }
    count = clusters if axes == "cluster" else members
    return {axes: lax.rem(lax.axis_index(axes) + k + 1, count)}


def stages(sizes):
    return ("both",) if sizes[0] * sizes[1] <= UNROLL else ("cluster", "sub")


class AllSum:
    def __init__(self, sizes, refs, n):
        self.spreads = []
        for i, axes in enumerate(stages(sizes)):
            source, slots, send, recv = refs[4 * i : 4 * i + 4]
            self.spreads.append(
                Spread(sizes, axes, source.at[n], slots.at[n], send.at[n], recv.at[n])
            )

    def start(self):
        self.spreads[0].start()

    def finish(self):
        for i, spread in enumerate(self.spreads):
            spread.wait_recv()
            out = total(spread.slots, spread.count, spread.source[...])
            if i + 1 < len(self.spreads):
                self.spreads[i + 1].source[...] = out
                self.spreads[i + 1].start()
        return out

    def wait_send(self):
        for spread in self.spreads:
            spread.wait_send()


def kernel(sizes, *refs):
    clusters, members = sizes
    hbm, out_ref, refs = refs[:9], refs[9], list(refs[10:])

    def take_refs(count):
        taken = refs[:count]
        del refs[:count]
        return taken

    local_refs = take_refs(9)
    (
        rhs_ref,
        ops_ref,
        signs_ref,
        links_ref,
        cluster_basis_ref,
        corner_basis_ref,
        ids_ref,
        cluster_coarse_ref,
        global_coarse_ref,
    ) = local_refs
    (local_sem,) = take_refs(1)
    basis_ref, basis_halves, swapped_basis, solve_ref, hot_ref = take_refs(5)
    corner_rows, corner_hot = take_refs(2)
    global_ref, picked_ref = take_refs(2)
    g_send, g_recv = take_refs(2)
    near_coarse, near_send, near_recv = take_refs(3)
    cross_refs = take_refs(4)
    (cross_image,) = take_refs(1)
    (share_ref,) = take_refs(1)
    share_refs = [take_refs(3) for _ in range(2)]
    sum_refs = [take_refs(4 * len(stages(sizes))) for _ in range(ITERS)]
    curve_refs = take_refs(4 * len(stages(sizes)))
    swap_refs = take_refs(8)
    table_refs = take_refs(8)

    subs, loads, dual = rhs_ref.shape
    rows = subs * loads
    kc, corn = cluster_basis_ref.shape[1], corner_basis_ref.shape[1]
    width = kc + corn
    coefs = subs * width
    order = global_coarse_ref.shape[1]
    solved = members * coefs
    near = share_refs[0][0].shape[2]
    my_c, my_s = lax.axis_index("cluster"), lax.axis_index("sub")
    has_low, has_high = my_s > 0, my_s < members - 1
    has_prev, has_next = my_c > 0, my_c < clusters - 1

    def run(copies, what, there=None):
        def act():
            for copy in copies:
                getattr(copy, what)()

        act() if there is None else pl.when(there)(act)


    barrier = pltpu.get_barrier_semaphore()

    def greet(device_id):
        pl.semaphore_signal(barrier, inc=1, device_id=device_id, device_id_type=MESH)

    greeted = 0
    for axes in ("both",) if len(stages(sizes)) == 1 else ("cluster", "sub"):
        count = peers_of(sizes, axes)
        each(count, lambda k, axes=axes: greet(peer(sizes, axes, k)))
        greeted += count
    if len(stages(sizes)) > 1:
        for there, step in ((has_next, 1), (has_prev, -1)):

            @pl.when(there)
            def _():
                for m in range(1, members):
                    greet({"cluster": my_c + step, "sub": lax.rem(my_s + m, members)})

            greeted = greeted + there.astype(jnp.int32) * (members - 1)

    loads_in = [
        pltpu.make_async_copy(hbm[i], local_refs[i], local_sem.at[i]) for i in range(len(hbm))
    ]
    for i in (6, 5, 4, 0, 7, 8, 3, 2, 1):
        loads_in[i].start()
    numbers = iota((8, LANES), 1).astype(jnp.bfloat16)

    loads_in[6].wait()
    id_row = jnp.full((1, coefs), -1, jnp.int32)
    lane = iota((1, coefs), 1)
    for s in range(subs):
        for c in range(corn):
            id_row = jnp.where(lane == s * width + kc + c, ids_ref[s, c], id_row)
    whose = iota((order, coefs), 0).astype(jnp.float32)
    corner_of = iota((coefs, order), 1).astype(jnp.float32)

    def hot_of(row):
        return (row == whose).astype(jnp.float32)

    def hot_rows(row):
        same = iota((coefs, coefs), 0) == iota((coefs, coefs), 1)
        column = jnp.sum(jnp.where(same, row, 0.0), axis=1, keepdims=True)
        return (column == corner_of).astype(jnp.float32)

    def corners_only(x):
        return jnp.concatenate(
            [x[s * width + kc : (s + 1) * width] for s in range(subs)], axis=0
        )

    def put_corners(i, row, x):
        at = slice(i * subs * corn, (i + 1) * subs * corn)
        corner_hot[at] = corners_only(hot_rows(row)).astype(jnp.bfloat16)
        x = corners_only(x)
        if i > 0:
            none = jnp.zeros(x.shape, jnp.float32)
            x = jnp.concatenate([x if b == i - 1 else none for b in range(3)], axis=1)
        put(corner_rows, (at,), x)

    hot_ref[...] = hot_rows(id_row.astype(jnp.float32)).astype(jnp.bfloat16)

    loads_in[5].wait()
    loads_in[4].wait()
    for s in range(subs):
        basis_ref[s * width : s * width + kc, :] = cluster_basis_ref[s]
        basis_ref[s * width + kc : (s + 1) * width, :] = corner_basis_ref[s]
    put(basis_halves, (), basis_ref[...])
    put_corners(0, id_row.astype(jnp.float32), basis_ref[...])

    where_to = iota((1, solved), 1)
    within = lax.rem(where_to, width)
    source = (where_to // coefs) * (subs * kc) + (lax.rem(where_to, coefs) // width) * kc + within
    source = jnp.where(within < kc, source, -1)
    place = (iota((members * subs * kc, solved), 0) == source).astype(jnp.float32)
    place = place.astype(jnp.bfloat16)

    def placed(x):
        return [dot(half, place, NN, None).astype(jnp.bfloat16) for half in halves(x)]

    solve_ref[...] = jnp.zeros(solve_ref.shape, jnp.bfloat16)

    def put_solve(first, x):
        for i, half in enumerate(placed(x)):
            for s in range(subs):
                at = first + s * width
                solve_ref[i, at : at + kc] = half[s * kc : (s + 1) * kc]

    loads_in[0].wait()
    loads_in[7].wait()
    put_solve(0, cluster_coarse_ref[0])

    diagonal = iota((rows, coefs), 0) // loads == iota((rows, coefs), 1) // width
    row_sub, lane_sub = iota((rows, coefs), 0) // loads, iota((rows, coefs), 1) // width
    crossed = row_sub + 1 - 2 * lax.rem(row_sub, 2) == lane_sub
    corner_at = iota((rows, 4 * subs * corn), 1)
    corner_sub = lax.rem(corner_at, subs * corn) // corn
    here = iota(corner_at.shape, 0) // loads
    across_sub = here + 1 - 2 * lax.rem(here, 2)
    corner_lanes = corner_sub == jnp.where(corner_at < 3 * subs * corn, here, across_sub)
    inner, outer = slice(0, 2 * LANES), slice(2 * LANES, dual)

    def per_load(x):
        out = x[:loads]
        for s in range(1, subs):
            out = out + x[s * loads : (s + 1) * loads]
        return out

    def lanes_added(x):
        out = x[:, :LANES]
        for b in range(1, dual // LANES):
            out = out + x[:, b * LANES : (b + 1) * LANES]
        return out

    def tiled(x):
        return jnp.concatenate([x] * subs, axis=0)

    def as_row(x):
        shape = (x.shape[0], LANES)
        sums = jnp.sum(x, axis=1, keepdims=True)
        kept = jnp.where(iota(shape, 0) == iota(shape, 1), sums, 0.0)
        return jnp.sum(kept, axis=0, keepdims=True)

    def as_column(x, first=0):
        mine = iota((rows, LANES), 1) == lax.rem(iota((rows, LANES), 0), loads) + first
        return jnp.sum(jnp.where(mine, x, 0.0), axis=1, keepdims=True)

    def dots(*products):
        return as_row(jnp.concatenate([per_load(lanes_added(x)) for x in products], axis=0))

    open_sends = []

    def first_near(member):
        return jnp.clip(member - 1, 0, members - near)

    def near_part(ref, target):
        return ref.at[pl.ds(first_near(target), near)]

    def push(refs, at, source, step, target):
        slots, send, recv = refs
        device_id = {"sub": target}
        if step:
            device_id["cluster"] = my_c + step
        return pltpu.make_async_remote_copy(
            src_ref=source,
            dst_ref=slots.at[at],
            send_sem=send.at[at],
            recv_sem=recv.at[at],
            device_id=device_id,
            device_id_type=MESH,
        )

    class Shares:
        def __init__(self, n):
            own, pieces = share_refs
            self.n = n
            mine = share_ref.at[n]

            def target(k):
                return lax.rem(my_s + k, members)

            def copies(refs, lead, of, step, ks):
                return [push(refs, lead + (k,), of(target(k)), step, target(k)) for k in ks]

            near_mine = functools.partial(near_part, mine)
            self.near = copies(own, (n,), near_mine, 0, range(1, members))
            self.sides = [
                copies(pieces, (n, side), lambda t: mine.at[t], 1 - 2 * side, range(members))
                for side in range(2)
            ]

        def start(self):
            self.run_sides("start", has_next, has_prev)
            run(self.near, "start")

        def wait_send(self):
            self.run_sides("wait_send", has_next, has_prev)
            run(self.near, "wait_send")

        def run_sides(self, what, *theres):
            for copies, there in zip(self.sides, theres):
                run(copies, what, there)

        def sum_of(self, terms):
            while len(terms) > 1:
                terms = [sum(terms[i : i + 2][1:], terms[i]) for i in range(0, len(terms), 2)]
            return terms[0]

        def of_near(self):
            for copy in self.near:
                copy.wait_recv()
            slots, base = share_refs[0][0], first_near(my_s)

            def of_member(member):
                near_slots = [slots[self.n, k, member - base] for k in range(1, members)]
                return self.sum_of([share_ref[self.n, member]] + near_slots)

            high = of_member(jnp.minimum(my_s + 1, members - 1))
            low = of_member(jnp.maximum(my_s - 1, 0))
            return of_member(my_s), high, low

        def of_sides(self):
            self.run_sides("wait_recv", has_prev, has_next)
            slots = share_refs[1][0]
            prev, following = [
                self.sum_of([slots[self.n, side, k] for k in range(members)]) for side in range(2)
            ]
            odd = lax.rem(iota((loads, coefs), 1) // width, 2) == 1
            following = jnp.where(has_next, following, 0.0)
            return jnp.where(odd, following, jnp.where(has_prev, prev, 0.0))

    def sums(n, raw, corner_raw, hot, row):
        tail_refs = sum_refs[n]
        tail_refs[0][0, :loads] = dot2(corner_raw, hot)
        if row is not None:
            tail_refs[0][0, loads:, :LANES] = row
            if order > LANES:
                tail_refs[0][0, loads:, LANES:] = jnp.zeros((1, order - LANES), jnp.float32)
        tail = AllSum(sizes, tail_refs, 0)
        share = Shares(n)

        def solve():
            share_out(n, jnp.concatenate(raw, axis=1))

        return tail, share, solve

    def share_out(n, inside):
        out = dot3(inside, [solve_ref[i, : inside.shape[1]] for i in range(2)])
        for j in range(members):
            share_ref[n, j] = out[:, j * coefs : (j + 1) * coefs]

    def block_diagonal(x, mask):
        return jnp.where(mask, tiled(x), 0.0)

    def raw_of(halved, lanes, b, mask):
        both, high = halved
        out = dot(both[:, lanes], b[0], NT, None)
        x = out[:rows] + out[rows:] + dot(high[:, lanes], b[1], NT, None)
        return per_load(jnp.where(mask, x, 0.0))

    def own_raw(halved):
        return raw_of(halved, slice(0, dual), basis_halves, diagonal)

    def swapped_raw(halved, i, lanes):
        b = [swapped_basis[0, i], swapped_basis[1, i]]
        return raw_of(halved, lanes, b, crossed if i == 2 else diagonal)

    def correction(tail, share, late=None):
        own, high, low = share.of_near()
        cross = share.of_sides()
        if late is not None:
            own, high, low = [x + y for x, y in zip((own, high, low), late.of_near())]
            open_sends.append(late)
        summed = tail.finish()
        out = dot3(summed[:loads], picked_ref)
        near = [x + out[:, i * coefs : (i + 1) * coefs] for i, x in enumerate((own, high, low))]
        open_sends.extend([tail, share])
        masked = [block_diagonal(x, diagonal) for x in near]
        fix = dot3(masked[0], basis_halves)
        swapped = [
            dot3(masked[i + 1], [swapped_basis[0, i], swapped_basis[1, i]]) for i in range(2)
        ]

        def last():
            total = cross + out[:, 3 * coefs :]
            if late is not None:
                total = total + late.of_sides()
            masked = block_diagonal(total, crossed)
            return dot3(masked, [swapped_basis[0, 2], swapped_basis[1, 2]]), masked

        return fix, jnp.concatenate(swapped, axis=1), last, summed[loads:, :LANES]

    def image_of(spread, depth, columns):
        out = None
        for s in range(subs):
            x = dot(spread, ops_ref[s, depth, columns], NN, None)
            if x.shape[0] > rows:
                x = x[:rows] + x[rows:]
            out = x if out is None else jnp.where(iota(x.shape, 0) // loads == s, x, out)
        return out

    def take(x, order_of):
        return jnp.take_along_axis(x, order_of, axis=1, mode="promise_in_bounds")

    class Swap:
        def __init__(self, refs, n):
            in_src, in_slots, in_send, in_recv, out_src, out_slots, out_send, out_recv = refs
            self.sources = [in_src.at[n, 0], in_src.at[n, 1], out_src.at[n, 0], out_src.at[n, 1]]
            self.slots = [
                in_slots.at[n, 0],
                in_slots.at[n, 1],
                out_slots.at[n, 0],
                out_slots.at[n, 1],
            ]
            self.send = [in_send.at[n, 0], in_send.at[n, 1], out_send.at[n, 0], out_send.at[n, 1]]
            self.recv = [in_recv.at[n, 0], in_recv.at[n, 1], out_recv.at[n, 0], out_recv.at[n, 1]]
            self.sends = [has_high, has_low, has_next, has_prev]
            self.takes = [has_low, has_high, has_prev, has_next]

        def copy(self, i):
            axis = "sub" if i < 2 else "cluster"
            return pltpu.make_async_remote_copy(
                src_ref=self.sources[i],
                dst_ref=self.slots[i],
                send_sem=self.send[i],
                recv_sem=self.recv[i],
                device_id={axis: lax.axis_index(axis) + (-1 if i % 2 else 1)},
                device_id_type=MESH,
            )

        def fill(self, x, orders, height, extra=None):
            up_order, down_order, across_order = orders
            count = subs * height
            across = take(x[:, 2 * LANES :], across_order)
            for p in range(2):
                for h in range(subs // 2):
                    s = 2 * h + p
                    self.sources[2 + p][h * height : (h + 1) * height] = across[
                        s * height : (s + 1) * height
                    ]
            self.sources[0][:count] = take(x[:, :LANES], up_order)
            self.sources[1][:count] = take(x[:, LANES : 2 * LANES], down_order)
            if extra is not None:
                for i in range(4):
                    first = count if i < 2 else count // 2
                    self.sources[i][first : first + 8] = extra

        def start(self):
            for i in (2, 3, 0, 1):
                pl.when(self.sends[i])(self.copy(i).start)

        def wait_recv(self, which=range(4)):
            for i in which:
                pl.when(self.takes[i])(self.copy(i).wait_recv)

        def wait_send(self):
            for i in range(4):
                pl.when(self.sends[i])(self.copy(i).wait_send)

        def arrived(self, i):
            return jnp.where(self.takes[i], self.slots[i][...], 0.0)

        def field(self):
            at_odd, at_even = self.arrived(2), self.arrived(3)
            across = [
                (at_odd if s % 2 else at_even)[s // 2 * loads : (s // 2 + 1) * loads]
                for s in range(subs)
            ]
            return jnp.concatenate(
                [self.arrived(1), self.arrived(0), jnp.concatenate(across, axis=0)], axis=1
            )

    depth = global_coarse_ref.shape[0]
    own_rows = pl.ds(pl.multiple_of(my_s * depth, 8), depth)

    def gather_copy(k):
        return pltpu.make_async_remote_copy(
            src_ref=global_coarse_ref,
            dst_ref=global_ref.at[own_rows],
            send_sem=g_send.at[k],
            recv_sem=g_recv.at[k],
            device_id=peer(sizes, "sub", k),
            device_id_type=MESH,
        )

    def near_copy(slot):
        return pltpu.make_async_remote_copy(
            src_ref=cluster_coarse_ref.at[0],
            dst_ref=near_coarse.at[slot],
            send_sem=near_send.at[slot],
            recv_sem=near_recv.at[slot],
            device_id={"sub": my_s + (1 if slot else -1)},
            device_id_type=MESH,
        )

    def cross_copy(slot):
        there, step = (has_prev, -1) if slot else (has_next, 1)
        lands = jnp.where(there, slot, slot + 2)
        return pltpu.make_async_remote_copy(
            src_ref=cross_refs[0],
            dst_ref=cross_refs[1].at[lands],
            send_sem=cross_refs[2].at[slot],
            recv_sem=cross_refs[3].at[lands],
            device_id={"cluster": my_c + jnp.where(there, step, -step)},
            device_id_type=MESH,
        )

    def cross_wait(slot, there):
        copy = pltpu.make_async_remote_copy(
            src_ref=cross_refs[0],
            dst_ref=cross_refs[1].at[slot],
            send_sem=cross_refs[2].at[slot % 2],
            recv_sem=cross_refs[3].at[slot],
            device_id={"cluster": my_c},
            device_id_type=MESH,
        )
        pl.when(there)(copy.wait_recv)

    coarse_copies = [near_copy(0), near_copy(1)]
    cross_copies = [cross_copy(0), cross_copy(1)]

    def plain(row):
        return row

    def inverted(row):
        hot = (iota((LANES, LANES), 0) == row).astype(jnp.float32).astype(jnp.bfloat16)
        return dot(numbers, hot, NT, None)[:1].astype(jnp.int32)

    loads_in[3].wait()
    index = [
        [inverted(links_ref[0, s : s + 1, :]) for s in range(subs)],
        [plain(links_ref[1, s : s + 1, :]) for s in range(subs)],
        [(plain if s % 2 else inverted)(links_ref[2, s : s + 1, :]) for s in range(subs)],
    ]

    def orders_of(height):
        return [
            jnp.concatenate([jnp.broadcast_to(row, (height, LANES)) for row in block], axis=0)
            for block in index
        ]

    rhs = jnp.concatenate([rhs_ref[s] for s in range(subs)], axis=0)
    orders = orders_of(loads)
    rhs_swap, tables = Swap(swap_refs, ITERS), Swap(table_refs, 0)
    rhs_swap.fill(rhs, orders, loads)
    ids_sent = jnp.broadcast_to(id_row.astype(jnp.float32), (8, coefs))
    tables.fill(basis_ref[...], orders_of(width), width, ids_sent)
    raw = [own_raw(stacked(rhs))]
    tail, share, solve = sums(0, raw, raw[0], hot_ref[...], None)
    solve()
    loads_in[8].wait()
    global_ref[own_rows, :] = global_coarse_ref[...]
    pl.semaphore_wait(barrier, greeted)
    tail.start()
    tables.start()
    share.start()
    rhs_swap.start()
    each(members - 1, lambda k: gather_copy(k).start())
    run(coarse_copies[:1], "start", has_low)
    run(coarse_copies[1:], "start", has_high)

    loads_in[2].wait()
    sign = jnp.concatenate(
        [
            jnp.broadcast_to(signs_ref[s : s + 1, :].astype(jnp.float32), (loads, dual))
            for s in range(subs)
        ],
        axis=0,
    )
    row_odd = lax.rem(iota((rows, LANES), 0) // loads, 2) == 1
    there = jnp.concatenate(
        [
            jnp.full((rows, LANES), has_high.astype(jnp.float32)),
            jnp.full((rows, LANES), has_low.astype(jnp.float32)),
            jnp.where(row_odd, has_prev.astype(jnp.float32), has_next.astype(jnp.float32)),
        ],
        axis=1,
    )
    loads_in[1].wait()
    open_sends.extend([rhs_swap, tables])
    each(members - 1, lambda k: gather_copy(k).wait_recv())
    partner = [s + 1 - 2 * (s % 2) for s in range(subs)]
    own_ids = id_row.astype(jnp.float32)

    def pick(first, id_rows):
        picks = jnp.concatenate([hot_of(row) for row in id_rows], axis=1).astype(jnp.bfloat16)
        lanes = slice(first * coefs, (first + len(id_rows)) * coefs)
        for r in range(0, order, 2 * LANES):
            chunk = slice(r, min(r + 2 * LANES, order))
            for i, half in enumerate(halves(global_ref[chunk])):
                picked_ref[i, chunk, lanes] = dot(half, picks, NN, None).astype(jnp.bfloat16)

    tables.wait_recv(range(2))
    arrived = [tables.arrived(1)[:coefs], tables.arrived(0)[:coefs]]
    for i in range(2):
        put(swapped_basis, (i,), arrived[i])
    id_rows = [own_ids] + [tables.slots[i][coefs : coefs + 1] for i in (1, 0)]
    pick(0, id_rows)
    for i in range(1, 3):
        put_corners(i, id_rows[i], arrived[i - 1])
    rhs_swap.wait_recv(range(2))
    tables.wait_recv(range(2, 4))
    from_prev, from_next = tables.arrived(2), tables.arrived(3)
    across = [
        (from_next if s % 2 else from_prev)[s // 2 * width : (s // 2 + 1) * width]
        for s in range(subs)
    ]
    across = jnp.concatenate(across, axis=0)
    put(swapped_basis, (2,), across)
    odd = lax.rem(lane // width, 2) == 1
    cross_ids = [tables.slots[i][coefs // 2 : coefs // 2 + 1] for i in (3, 2)]
    cross_ids = jnp.where(odd, *cross_ids)
    pick(3, [cross_ids])
    put_corners(3, cross_ids, across)
    across = across * jnp.concatenate(
        [
            jnp.broadcast_to(sign[loads * s : loads * s + 1, outer], (width, LANES))
            for s in partner
        ],
        axis=0,
    )
    rhs_swap.wait_recv(range(2, 4))
    rhs_swapped = rhs_swap.field()

    fix, fix_swapped, last, _ = correction(tail, share)
    fix_swapped = jnp.concatenate([fix_swapped, last()[0]], axis=1)
    direction = rhs - fix
    direction_swapped = rhs_swapped - fix_swapped
    spread = sign * (direction + direction_swapped)
    spread_bf = spread.astype(jnp.bfloat16)
    everything = slice(0, dual)
    image = image_of(spread_bf, everything, outer)
    rest = image_of(spread_bf, everything, inner)
    cross = swapped_raw(stacked(sign[:, outer] * image), 2, slice(0, LANES))
    image = jnp.concatenate([rest, image], axis=1)
    signed = sign * image
    halved = stacked(signed)
    corner_raw = raw_of(halved, everything, corner_rows, corner_lanes)
    raw = [own_raw(halved)]
    raw += [swapped_raw(halved, i, slice(i * LANES, (i + 1) * LANES)) for i in range(2)]
    cross_refs[0][...] = cross
    run(cross_copies, "start")
    tail, share, solve = sums(1, raw, corner_raw, corner_hot[...], dots(spread * image, rhs * rhs))
    tail.start()
    run(coarse_copies[:1], "wait_recv", has_high)
    run(coarse_copies[1:], "wait_recv", has_low)
    for slot, has in enumerate((has_high, has_low)):
        put_solve((slot + 1) * coefs, jnp.where(has, near_coarse[slot], 0.0))
    solve()
    share.start()
    for s in range(subs):
        mine = slice(partner[s] * width, (partner[s] + 1) * width)
        x = dot(stacked(across[mine])[0], ops_ref[s, outer, :], NN, None)
        put(cross_image, (mine,), x[:width] + x[width:])
    swap = Swap(swap_refs, 0)
    swap.fill(signed, orders, loads)
    swap.start()
    cross_wait(0, has_prev)
    cross_wait(1, has_next)
    from_prev = jnp.where(has_prev, cross_refs[1][0], 0.0)
    from_next = jnp.where(has_next, cross_refs[1][1], 0.0)
    share_out(2, jnp.where(odd, from_prev, from_next))
    late = Shares(2)
    late.start()
    swap.wait_recv()
    signed_swapped = swap.field()
    product = signed + signed_swapped
    product_swapped = signed_swapped + there * signed

    fix, fix_swapped, last, row = correction(tail, share, late)
    curvature, rho = as_column(row), as_column(row, loads)
    step = rho / curvature
    residual = rhs - step * product
    moved = direction - step * (product - fix)

    fix_swapped = jnp.concatenate([fix_swapped, jnp.zeros((rows, LANES), jnp.float32)], axis=1)
    moved_swapped = direction_swapped - step * (product_swapped - fix_swapped)
    spread_moved = sign * (moved + moved_swapped)
    image_moved = image_of(stacked(spread_moved)[0], everything, everything)
    last_fix, masked = last()
    image_moved = image_moved + step * dot3(masked, cross_image)
    last_fix = step * sign[:, outer] * last_fix
    spread_moved = jnp.concatenate(
        [spread_moved[:, inner], spread_moved[:, outer] + last_fix], axis=1
    )
    curve_refs[0][0] = dots(
        residual * residual,
        spread_moved * image_moved,
        spread_moved * image + spread * image_moved,
    )
    curve = AllSum(sizes, curve_refs, 0)
    curve.start()
    signed = sign * image_moved
    last_swap = Swap(swap_refs, 1)
    last_swap.fill(signed, orders, loads)
    last_swap.start()
    last_swap.wait_recv()
    product_moved = signed + last_swap.field()
    for spread in open_sends + [swap]:
        spread.wait_send()
    each(members - 1, lambda k: gather_copy(k).wait_send())
    run(coarse_copies[:1], "wait_send", has_low)
    run(coarse_copies[1:], "wait_send", has_high)
    run(cross_copies, "wait_send")
    cross_wait(2, my_c == clusters - 2)
    cross_wait(3, my_c == 1)
    row = curve.finish()
    ratio = as_column(row) / rho
    last_curvature = as_column(row, loads) + ratio * (
        as_column(row, 2 * loads) + ratio * curvature
    )
    last_step = ratio * rho / last_curvature
    multipliers = (step + last_step * ratio) * direction + last_step * moved
    residual = residual - last_step * (product_moved + ratio * product)
    for s in range(subs):
        out_ref[0, s] = multipliers[s * loads : (s + 1) * loads]
        out_ref[1, s] = residual[s * loads : (s + 1) * loads]
    curve.wait_send()
    last_swap.wait_send()


def split(both_ref, mult_ref, res_ref, sems):
    copies = [
        pltpu.make_async_copy(both_ref.at[i], out, sems.at[i])
        for i, out in enumerate((mult_ref, res_ref))
    ]
    for copy in copies:
        copy.start()
    for copy in copies:
        copy.wait()


def local(sizes, *args):
    args = list(args)
    args[3] = jnp.transpose(args[3], (1, 0, 2))
    rhs, operators, signs, links, cluster_basis, corner_basis, ids, coarse, glob = args
    clusters, members = sizes
    subs, loads, dual = rhs.shape
    corn = corner_basis.shape[1]
    coefs = subs * (cluster_basis.shape[1] + corn)
    depth, order = glob.shape
    f32 = jnp.float32
    dma = pltpu.SemaphoreType.DMA

    def exchange(lead, block, receive):
        return [
            pltpu.VMEM(lead[:1] + block, f32),
            pltpu.VMEM(lead + receive, f32),
            dma(lead),
            dma(lead),
        ]

    def swap_scratch(count, height, extra):
        scratch = []
        for rows in (subs * height + extra, subs * height // 2 + extra):
            scratch += [
                pltpu.VMEM((count, 2, rows, LANES), f32),
                pltpu.VMEM((count, 2, rows, LANES), f32),
                dma((count, 2)),
                dma((count, 2)),
            ]
        return scratch

    def sum_scratch(count, block):
        scratch = []
        for axes in stages(sizes):
            scratch += exchange((count, peers_of(sizes, axes)), block, block)
        return scratch

    vmem = pl.BlockSpec(memory_space=pltpu.VMEM)
    scratch = [pltpu.VMEM(a.shape, a.dtype) for a in args]
    scratch[6] = pltpu.SMEM(ids.shape, ids.dtype)
    bf16 = jnp.bfloat16
    solved = members * coefs
    inside, columns = coarse.shape[1:]
    scratch += [
        dma((len(args),)),
        pltpu.VMEM((coefs, dual), f32),
        pltpu.VMEM((2, coefs, dual), bf16),
        pltpu.VMEM((2, 3, coefs, LANES), bf16),
        pltpu.VMEM((2, 3 * coefs, solved), bf16),
        pltpu.VMEM((coefs, order), bf16),
        pltpu.VMEM((2, 4 * subs * corn, dual), bf16),
        pltpu.VMEM((4 * subs * corn, order), bf16),
        pltpu.VMEM((order, order), f32),
        pltpu.VMEM((2, order, 4 * coefs), bf16),
        dma((members - 1,)),
        dma((members - 1,)),
        pltpu.VMEM((2, inside, columns), f32),
        dma((2,)),
        dma((2,)),
        pltpu.VMEM((loads, coefs), f32),
        pltpu.VMEM((4, loads, coefs), f32),
        dma((2,)),
        dma((4,)),
        pltpu.VMEM((2, coefs, dual), bf16),
        pltpu.VMEM((ITERS + 1, members, loads, coefs), f32),
    ]
    block, near = (loads, coefs), (min(3, members), loads, coefs)
    for lead, shape in (
        ((ITERS + 1, members), near),
        ((ITERS + 1, 2, members), block),
    ):
        scratch += [pltpu.VMEM(lead + shape, f32), dma(lead), dma(lead)]
    scratch += sum_scratch(1, (loads, order)) + sum_scratch(1, (loads + 1, order))
    scratch += sum_scratch(1, (1, LANES))
    scratch += swap_scratch(ITERS + 1, loads, 0)
    scratch += swap_scratch(1, coefs // subs, 8)
    both = pl.pallas_call(
        functools.partial(kernel, sizes),
        out_shape=pltpu.VMEM((2,) + rhs.shape, f32),
        in_specs=[pl.BlockSpec(memory_space=pltpu.HBM)] * len(args),
        out_specs=vmem,
        scratch_shapes=scratch,
        compiler_params=pltpu.CompilerParams(
            collective_id=0, has_side_effects=True, vmem_limit_bytes=56 << 20
        ),
    )(*args)
    return pl.pallas_call(
        split,
        out_shape=[jax.ShapeDtypeStruct(rhs.shape, f32)] * 2,
        in_specs=[vmem],
        out_specs=[pl.BlockSpec(memory_space=pltpu.HBM)] * 2,
        scratch_shapes=[dma((2,))],
        compiler_params=pltpu.CompilerParams(vmem_limit_bytes=4 << 20),
    )(both)


def solution(mesh):
    placed = (
        P(("cluster", "sub"), None, None),
        P(("cluster", "sub"), None, None),
        P(("cluster", "sub"), None),
        P(("cluster", "sub"), None, None),
        P(("cluster", "sub"), None, None),
        P(("cluster", "sub"), None, None),
        P(("cluster", "sub"), None),
        P("cluster", "sub", None),
        P("sub", None),
    )
    return jax.shard_map(
        functools.partial(local, (mesh.shape["cluster"], mesh.shape["sub"])),
        mesh=mesh,
        in_specs=placed,
        out_specs=(P(("cluster", "sub"), None, None), P(("cluster", "sub"), None, None)),
        check_vma=False,
    )
```

```python
import functools

import jax
import jax.numpy as jnp
from jax import lax
from jax.experimental import pallas as pl
from jax.experimental.pallas import tpu as pltpu
from jax.sharding import PartitionSpec as P

ITERS = 2
LANES = 128
UNROLL = 32
MESH = pl.DeviceIdType.MESH
HIGHEST = lax.Precision.HIGHEST
NN = (((1,), (0,)), ((), ()))
NT = (((1,), (1,)), ((), ()))


def dot(a, b, dims=NN, precision=HIGHEST):
    return lax.dot_general(a, b, dims, precision=precision, preferred_element_type=jnp.float32)


def halves(x):
    high = x.astype(jnp.bfloat16)
    return high, (x - high.astype(jnp.float32)).astype(jnp.bfloat16)


def stacked(a):
    high = a.astype(jnp.bfloat16).astype(jnp.float32)
    return jnp.concatenate([high, a - high], axis=0).astype(jnp.bfloat16), high.astype(jnp.bfloat16)


def dot2(a, b, dims=NN):
    rows = a.shape[0]
    out = dot(stacked(a)[0], b, dims, None)
    return out[:rows] + out[rows:]


def dot3(a, b, dims=NN):
    rows = a.shape[0]
    both, high = stacked(a)
    out = dot(both, b[0], dims, None)
    return out[:rows] + out[rows:] + dot(high, b[1], dims, None)


def put(ref, index, x):
    for i, half in enumerate(halves(x)):
        ref[(i,) + index] = half


def iota(shape, dim):
    return lax.broadcasted_iota(jnp.int32, shape, dim)


def each(count, body):
    if count <= UNROLL:
        for k in range(count):
            body(k)
    else:
        lax.fori_loop(0, count, lambda k, carry: (body(k), carry)[1], 0)


def total(ref, count, start):
    if count <= UNROLL:
        terms = [start] + [ref[k] for k in range(count)]
        while len(terms) > 1:
            terms = [sum(terms[i : i + 2][1:], terms[i]) for i in range(0, len(terms), 2)]
        return terms[0]
    return lax.fori_loop(0, count, lambda k, acc: acc + ref[k], start)


class Spread:
    def __init__(self, sizes, axes, source, slots, send, recv):
        self.sizes, self.axes = sizes, axes
        self.source, self.slots, self.send, self.recv = source, slots, send, recv
        self.count = peers_of(sizes, axes)

    def copy(self, k):
        return pltpu.make_async_remote_copy(
            src_ref=self.source,
            dst_ref=self.slots.at[k],
            send_sem=self.send.at[k],
            recv_sem=self.recv.at[k],
            device_id=peer(self.sizes, self.axes, k),
            device_id_type=MESH,
        )

    def start(self):
        each(self.count, lambda k: self.copy(k).start())

    def wait_recv(self):
        each(self.count, lambda k: self.copy(k).wait_recv())

    def wait_send(self):
        each(self.count, lambda k: self.copy(k).wait_send())


def peers_of(sizes, axes):
    clusters, members = sizes
    return {"both": clusters * members, "cluster": clusters, "sub": members}[axes] - 1


def peer(sizes, axes, k):
    clusters, members = sizes
    if axes == "both":
        c, m = (k + 1) // members, (k + 1) % members
        return {
            "cluster": lax.rem(lax.axis_index("cluster") + c, clusters),
            "sub": lax.rem(lax.axis_index("sub") + m, members),
        }
    count = clusters if axes == "cluster" else members
    return {axes: lax.rem(lax.axis_index(axes) + k + 1, count)}


def stages(sizes):
    return ("both",) if sizes[0] * sizes[1] <= UNROLL else ("cluster", "sub")


class AllSum:
    def __init__(self, sizes, refs, n):
        self.spreads = []
        for i, axes in enumerate(stages(sizes)):
            source, slots, send, recv = refs[4 * i : 4 * i + 4]
            self.spreads.append(
                Spread(sizes, axes, source.at[n], slots.at[n], send.at[n], recv.at[n])
            )

    def start(self):
        self.spreads[0].start()

    def finish(self):
        for i, spread in enumerate(self.spreads):
            spread.wait_recv()
            out = total(spread.slots, spread.count, spread.source[...])
            if i + 1 < len(self.spreads):
                self.spreads[i + 1].source[...] = out
                self.spreads[i + 1].start()
        return out

    def wait_send(self):
        for spread in self.spreads:
            spread.wait_send()


def kernel(sizes, *refs):
    clusters, members = sizes
    hbm, out_ref, refs = refs[:9], refs[9], list(refs[10:])

    def take_refs(count):
        taken = refs[:count]
        del refs[:count]
        return taken

    local_refs = take_refs(9)
    (
        rhs_ref,
        ops_ref,
        signs_ref,
        links_ref,
        cluster_basis_ref,
        corner_basis_ref,
        ids_ref,
        cluster_coarse_ref,
        global_coarse_ref,
    ) = local_refs
    (local_sem,) = take_refs(1)
    basis_ref, basis_halves, swapped_basis, solve_ref, hot_ref = take_refs(5)
    corner_rows, corner_hot = take_refs(2)
    global_ref, picked_ref = take_refs(2)
    g_send, g_recv = take_refs(2)
    near_coarse, near_send, near_recv = take_refs(3)
    cross_refs = take_refs(4)
    (cross_image,) = take_refs(1)
    (share_ref,) = take_refs(1)
    share_refs = [take_refs(3) for _ in range(2)]
    sum_refs = [take_refs(4 * len(stages(sizes))) for _ in range(ITERS)]
    curve_refs = take_refs(4 * len(stages(sizes)))
    swap_refs = take_refs(8)
    table_refs = take_refs(8)

    subs, loads, dual = rhs_ref.shape
    rows = subs * loads
    kc, corn = cluster_basis_ref.shape[1], corner_basis_ref.shape[1]
    width = kc + corn
    coefs = subs * width
    order = global_coarse_ref.shape[1]
    solved = members * coefs
    near = share_refs[0][0].shape[2]
    my_c, my_s = lax.axis_index("cluster"), lax.axis_index("sub")
    has_low, has_high = my_s > 0, my_s < members - 1
    has_prev, has_next = my_c > 0, my_c < clusters - 1

    def run(copies, what, there=None):
        def act():
            for copy in copies:
                getattr(copy, what)()

        act() if there is None else pl.when(there)(act)


    barrier = pltpu.get_barrier_semaphore()

    def greet(device_id):
        pl.semaphore_signal(barrier, inc=1, device_id=device_id, device_id_type=MESH)

    greeted = 0
    for axes in ("both",) if len(stages(sizes)) == 1 else ("cluster", "sub"):
        count = peers_of(sizes, axes)
        each(count, lambda k, axes=axes: greet(peer(sizes, axes, k)))
        greeted += count
    if len(stages(sizes)) > 1:
        for there, step in ((has_next, 1), (has_prev, -1)):

            @pl.when(there)
            def _():
                for m in range(1, members):
                    greet({"cluster": my_c + step, "sub": lax.rem(my_s + m, members)})

            greeted = greeted + there.astype(jnp.int32) * (members - 1)

    loads_in = [
        pltpu.make_async_copy(hbm[i], local_refs[i], local_sem.at[i]) for i in range(len(hbm))
    ]
    for i in (6, 5, 4, 0, 7, 8, 3, 2, 1):
        loads_in[i].start()
    numbers = iota((8, LANES), 1).astype(jnp.bfloat16)

    loads_in[6].wait()
    id_row = jnp.full((1, coefs), -1, jnp.int32)
    lane = iota((1, coefs), 1)
    for s in range(subs):
        for c in range(corn):
            id_row = jnp.where(lane == s * width + kc + c, ids_ref[s, c], id_row)
    whose = iota((order, coefs), 0).astype(jnp.float32)
    corner_of = iota((coefs, order), 1).astype(jnp.float32)

    def hot_of(row):
        return (row == whose).astype(jnp.float32)

    def hot_rows(row):
        same = iota((coefs, coefs), 0) == iota((coefs, coefs), 1)
        column = jnp.sum(jnp.where(same, row, 0.0), axis=1, keepdims=True)
        return (column == corner_of).astype(jnp.float32)

    def corners_only(x):
        return jnp.concatenate(
            [x[s * width + kc : (s + 1) * width] for s in range(subs)], axis=0
        )

    def put_corners(i, row, x):
        at = slice(i * subs * corn, (i + 1) * subs * corn)
        corner_hot[at] = corners_only(hot_rows(row)).astype(jnp.bfloat16)
        x = corners_only(x)
        if i > 0:
            none = jnp.zeros(x.shape, jnp.float32)
            x = jnp.concatenate([x if b == i - 1 else none for b in range(3)], axis=1)
        put(corner_rows, (at,), x)

    hot_ref[...] = hot_rows(id_row.astype(jnp.float32)).astype(jnp.bfloat16)

    loads_in[5].wait()
    loads_in[4].wait()
    for s in range(subs):
        basis_ref[s * width : s * width + kc, :] = cluster_basis_ref[s]
        basis_ref[s * width + kc : (s + 1) * width, :] = corner_basis_ref[s]
    put(basis_halves, (), basis_ref[...])
    put_corners(0, id_row.astype(jnp.float32), basis_ref[...])

    where_to = iota((1, solved), 1)
    within = lax.rem(where_to, width)
    source = (where_to // coefs) * (subs * kc) + (lax.rem(where_to, coefs) // width) * kc + within
    source = jnp.where(within < kc, source, -1)
    place = (iota((members * subs * kc, solved), 0) == source).astype(jnp.float32)
    place = place.astype(jnp.bfloat16)

    def placed(x):
        return [dot(half, place, NN, None).astype(jnp.bfloat16) for half in halves(x)]

    solve_ref[...] = jnp.zeros(solve_ref.shape, jnp.bfloat16)

    def put_solve(first, x):
        for i, half in enumerate(placed(x)):
            for s in range(subs):
                at = first + s * width
                solve_ref[i, at : at + kc] = half[s * kc : (s + 1) * kc]

    loads_in[0].wait()
    loads_in[7].wait()
    put_solve(0, cluster_coarse_ref[0])

    diagonal = iota((rows, coefs), 0) // loads == iota((rows, coefs), 1) // width
    row_sub, lane_sub = iota((rows, coefs), 0) // loads, iota((rows, coefs), 1) // width
    crossed = row_sub + 1 - 2 * lax.rem(row_sub, 2) == lane_sub
    corner_at = iota((rows, 4 * subs * corn), 1)
    corner_sub = lax.rem(corner_at, subs * corn) // corn
    here = iota(corner_at.shape, 0) // loads
    across_sub = here + 1 - 2 * lax.rem(here, 2)
    corner_lanes = corner_sub == jnp.where(corner_at < 3 * subs * corn, here, across_sub)
    inner, outer = slice(0, 2 * LANES), slice(2 * LANES, dual)

    def per_load(x):
        out = x[:loads]
        for s in range(1, subs):
            out = out + x[s * loads : (s + 1) * loads]
        return out

    def lanes_added(x):
        out = x[:, :LANES]
        for b in range(1, dual // LANES):
            out = out + x[:, b * LANES : (b + 1) * LANES]
        return out

    def tiled(x):
        return jnp.concatenate([x] * subs, axis=0)

    def as_row(x):
        shape = (x.shape[0], LANES)
        sums = jnp.sum(x, axis=1, keepdims=True)
        kept = jnp.where(iota(shape, 0) == iota(shape, 1), sums, 0.0)
        return jnp.sum(kept, axis=0, keepdims=True)

    def as_column(x, first=0):
        mine = iota((rows, LANES), 1) == lax.rem(iota((rows, LANES), 0), loads) + first
        return jnp.sum(jnp.where(mine, x, 0.0), axis=1, keepdims=True)

    def summed_lanes(x):
        return per_load(lanes_added(x)) if x.shape[0] == rows else x

    def dots(*products):
        return as_row(jnp.concatenate([summed_lanes(x) for x in products], axis=0))

    open_sends = []

    def first_near(member):
        return jnp.clip(member - 1, 0, members - near)

    def near_part(ref, target):
        return ref.at[pl.ds(first_near(target), near)]

    def push(refs, at, source, step, target):
        slots, send, recv = refs
        device_id = {"sub": target}
        if step:
            device_id["cluster"] = my_c + step
        return pltpu.make_async_remote_copy(
            src_ref=source,
            dst_ref=slots.at[at],
            send_sem=send.at[at],
            recv_sem=recv.at[at],
            device_id=device_id,
            device_id_type=MESH,
        )

    class Shares:
        def __init__(self, n):
            own, pieces = share_refs
            self.n = n
            mine = share_ref.at[n]

            def target(k):
                return lax.rem(my_s + k, members)

            def copies(refs, lead, of, step, ks):
                return [push(refs, lead + (k,), of(target(k)), step, target(k)) for k in ks]

            near_mine = functools.partial(near_part, mine)
            self.near = copies(own, (n,), near_mine, 0, range(1, members))
            self.sides = [
                copies(pieces, (n, side), lambda t: mine.at[t], 1 - 2 * side, range(members))
                for side in range(2)
            ]

        def start(self):
            self.run_sides("start", has_next, has_prev)
            run(self.near, "start")

        def wait_send(self):
            self.run_sides("wait_send", has_next, has_prev)
            run(self.near, "wait_send")

        def run_sides(self, what, *theres):
            for copies, there in zip(self.sides, theres):
                run(copies, what, there)

        def sum_of(self, terms):
            while len(terms) > 1:
                terms = [sum(terms[i : i + 2][1:], terms[i]) for i in range(0, len(terms), 2)]
            return terms[0]

        def of_near(self):
            for copy in self.near:
                copy.wait_recv()
            slots, base = share_refs[0][0], first_near(my_s)

            def of_member(member):
                near_slots = [slots[self.n, k, member - base] for k in range(1, members)]
                return self.sum_of([share_ref[self.n, member]] + near_slots)

            high = of_member(jnp.minimum(my_s + 1, members - 1))
            low = of_member(jnp.maximum(my_s - 1, 0))
            return of_member(my_s), high, low

        def of_sides(self):
            self.run_sides("wait_recv", has_prev, has_next)
            slots = share_refs[1][0]
            prev, following = [
                self.sum_of([slots[self.n, side, k] for k in range(members)]) for side in range(2)
            ]
            odd = lax.rem(iota((loads, coefs), 1) // width, 2) == 1
            following = jnp.where(has_next, following, 0.0)
            return jnp.where(odd, following, jnp.where(has_prev, prev, 0.0))

    def sums(n, raw, corner_raw, hot, row):
        tail_refs = sum_refs[n]
        tail_refs[0][0, :loads] = dot2(corner_raw, hot)
        if row is not None:
            tail_refs[0][0, loads:, :LANES] = row
            if order > LANES:
                tail_refs[0][0, loads:, LANES:] = jnp.zeros((1, order - LANES), jnp.float32)
        tail = AllSum(sizes, tail_refs, 0)
        share = Shares(n)

        def solve():
            share_out(n, jnp.concatenate(raw, axis=1))

        return tail, share, solve

    def share_out(n, inside):
        out = dot3(inside, [solve_ref[i, : inside.shape[1]] for i in range(2)])
        for j in range(members):
            share_ref[n, j] = out[:, j * coefs : (j + 1) * coefs]

    def block_diagonal(x, mask):
        return jnp.where(mask, tiled(x), 0.0)

    def raw_of(halved, lanes, b, mask):
        both, high = halved
        out = dot(both[:, lanes], b[0], NT, None)
        x = out[:rows] + out[rows:] + dot(high[:, lanes], b[1], NT, None)
        return per_load(jnp.where(mask, x, 0.0))

    def own_raw(halved):
        return raw_of(halved, slice(0, dual), basis_halves, diagonal)

    def swapped_raw(halved, i, lanes):
        b = [swapped_basis[0, i], swapped_basis[1, i]]
        return raw_of(halved, lanes, b, crossed if i == 2 else diagonal)

    def correction(tail, share, late=None):
        own, high, low = share.of_near()
        cross = share.of_sides()
        if late is not None:
            own, high, low = [x + y for x, y in zip((own, high, low), late.of_near())]
            open_sends.append(late)
        summed = tail.finish()
        out = dot3(summed[:loads], picked_ref)
        near = [x + out[:, i * coefs : (i + 1) * coefs] for i, x in enumerate((own, high, low))]
        open_sends.extend([tail, share])
        masked = [block_diagonal(x, diagonal) for x in near]
        fix = dot3(masked[0], basis_halves)
        swapped = [
            dot3(masked[i + 1], [swapped_basis[0, i], swapped_basis[1, i]]) for i in range(2)
        ]

        def last():
            total = cross + out[:, 3 * coefs :]
            if late is not None:
                total = total + late.of_sides()
            masked = block_diagonal(total, crossed)
            return dot3(masked, [swapped_basis[0, 2], swapped_basis[1, 2]]), masked

        return fix, jnp.concatenate(swapped, axis=1), last, summed[loads:, :LANES]

    def image_of(spread, depth, columns):
        out = None
        for s in range(subs):
            x = dot(spread, ops_ref[s, depth, columns], NN, None)
            if x.shape[0] > rows:
                x = x[:rows] + x[rows:]
            out = x if out is None else jnp.where(iota(x.shape, 0) // loads == s, x, out)
        return out

    def take(x, order_of):
        return jnp.take_along_axis(x, order_of, axis=1, mode="promise_in_bounds")

    class Swap:
        def __init__(self, refs, n):
            in_src, in_slots, in_send, in_recv, out_src, out_slots, out_send, out_recv = refs
            self.sources = [in_src.at[n, 0], in_src.at[n, 1], out_src.at[n, 0], out_src.at[n, 1]]
            self.slots = [
                in_slots.at[n, 0],
                in_slots.at[n, 1],
                out_slots.at[n, 0],
                out_slots.at[n, 1],
            ]
            self.send = [in_send.at[n, 0], in_send.at[n, 1], out_send.at[n, 0], out_send.at[n, 1]]
            self.recv = [in_recv.at[n, 0], in_recv.at[n, 1], out_recv.at[n, 0], out_recv.at[n, 1]]
            self.sends = [has_high, has_low, has_next, has_prev]
            self.takes = [has_low, has_high, has_prev, has_next]

        def copy(self, i):
            axis = "sub" if i < 2 else "cluster"
            return pltpu.make_async_remote_copy(
                src_ref=self.sources[i],
                dst_ref=self.slots[i],
                send_sem=self.send[i],
                recv_sem=self.recv[i],
                device_id={axis: lax.axis_index(axis) + (-1 if i % 2 else 1)},
                device_id_type=MESH,
            )

        def fill(self, x, orders, height, extra=None):
            up_order, down_order, across_order = orders
            count = subs * height
            across = take(x[:, 2 * LANES :], across_order)
            for p in range(2):
                for h in range(subs // 2):
                    s = 2 * h + p
                    self.sources[2 + p][h * height : (h + 1) * height] = across[
                        s * height : (s + 1) * height
                    ]
            self.sources[0][:count] = take(x[:, :LANES], up_order)
            self.sources[1][:count] = take(x[:, LANES : 2 * LANES], down_order)
            if extra is not None:
                for i in range(4):
                    first = count if i < 2 else count // 2
                    self.sources[i][first : first + 8] = extra

        def start(self):
            for i in (2, 3, 0, 1):
                pl.when(self.sends[i])(self.copy(i).start)

        def wait_recv(self, which=range(4)):
            for i in which:
                pl.when(self.takes[i])(self.copy(i).wait_recv)

        def wait_send(self):
            for i in range(4):
                pl.when(self.sends[i])(self.copy(i).wait_send)

        def arrived(self, i):
            return jnp.where(self.takes[i], self.slots[i][...], 0.0)

        def field(self):
            at_odd, at_even = self.arrived(2), self.arrived(3)
            across = [
                (at_odd if s % 2 else at_even)[s // 2 * loads : (s // 2 + 1) * loads]
                for s in range(subs)
            ]
            return jnp.concatenate(
                [self.arrived(1), self.arrived(0), jnp.concatenate(across, axis=0)], axis=1
            )

    depth = global_coarse_ref.shape[0]
    own_rows = pl.ds(pl.multiple_of(my_s * depth, 8), depth)

    def gather_copy(k):
        return pltpu.make_async_remote_copy(
            src_ref=global_coarse_ref,
            dst_ref=global_ref.at[own_rows],
            send_sem=g_send.at[k],
            recv_sem=g_recv.at[k],
            device_id=peer(sizes, "sub", k),
            device_id_type=MESH,
        )

    def near_copy(slot):
        return pltpu.make_async_remote_copy(
            src_ref=cluster_coarse_ref.at[0],
            dst_ref=near_coarse.at[slot],
            send_sem=near_send.at[slot],
            recv_sem=near_recv.at[slot],
            device_id={"sub": my_s + (1 if slot else -1)},
            device_id_type=MESH,
        )

    def cross_copy(slot):
        there, step = (has_prev, -1) if slot else (has_next, 1)
        lands = jnp.where(there, slot, slot + 2)
        return pltpu.make_async_remote_copy(
            src_ref=cross_refs[0],
            dst_ref=cross_refs[1].at[lands],
            send_sem=cross_refs[2].at[slot],
            recv_sem=cross_refs[3].at[lands],
            device_id={"cluster": my_c + jnp.where(there, step, -step)},
            device_id_type=MESH,
        )

    def cross_wait(slot, there):
        copy = pltpu.make_async_remote_copy(
            src_ref=cross_refs[0],
            dst_ref=cross_refs[1].at[slot],
            send_sem=cross_refs[2].at[slot % 2],
            recv_sem=cross_refs[3].at[slot],
            device_id={"cluster": my_c},
            device_id_type=MESH,
        )
        pl.when(there)(copy.wait_recv)

    coarse_copies = [near_copy(0), near_copy(1)]
    cross_copies = [cross_copy(0), cross_copy(1)]

    def plain(row):
        return row

    def inverted(row):
        hot = (iota((LANES, LANES), 0) == row).astype(jnp.float32).astype(jnp.bfloat16)
        return dot(numbers, hot, NT, None)[:1].astype(jnp.int32)

    loads_in[3].wait()
    index = [
        [inverted(links_ref[0, s : s + 1, :]) for s in range(subs)],
        [plain(links_ref[1, s : s + 1, :]) for s in range(subs)],
        [(plain if s % 2 else inverted)(links_ref[2, s : s + 1, :]) for s in range(subs)],
    ]

    def orders_of(height):
        return [
            jnp.concatenate([jnp.broadcast_to(row, (height, LANES)) for row in block], axis=0)
            for block in index
        ]

    rhs = jnp.concatenate([rhs_ref[s] for s in range(subs)], axis=0)
    orders = orders_of(loads)
    rhs_swap, tables = Swap(swap_refs, ITERS), Swap(table_refs, 0)
    rhs_swap.fill(rhs, orders, loads)
    ids_sent = jnp.broadcast_to(id_row.astype(jnp.float32), (8, coefs))
    tables.fill(basis_ref[...], orders_of(width), width, ids_sent)
    raw = [own_raw(stacked(rhs))]
    tail, share, solve = sums(0, raw, raw[0], hot_ref[...], None)
    solve()
    loads_in[8].wait()
    global_ref[own_rows, :] = global_coarse_ref[...]
    pl.semaphore_wait(barrier, greeted)
    tail.start()
    tables.start()
    share.start()
    rhs_swap.start()
    each(members - 1, lambda k: gather_copy(k).start())
    run(coarse_copies[:1], "start", has_low)
    run(coarse_copies[1:], "start", has_high)

    loads_in[2].wait()
    sign = jnp.concatenate(
        [
            jnp.broadcast_to(signs_ref[s : s + 1, :].astype(jnp.float32), (loads, dual))
            for s in range(subs)
        ],
        axis=0,
    )
    row_odd = lax.rem(iota((rows, LANES), 0) // loads, 2) == 1
    there = jnp.concatenate(
        [
            jnp.full((rows, LANES), has_high.astype(jnp.float32)),
            jnp.full((rows, LANES), has_low.astype(jnp.float32)),
            jnp.where(row_odd, has_prev.astype(jnp.float32), has_next.astype(jnp.float32)),
        ],
        axis=1,
    )
    loads_in[1].wait()
    open_sends.extend([rhs_swap, tables])
    each(members - 1, lambda k: gather_copy(k).wait_recv())
    partner = [s + 1 - 2 * (s % 2) for s in range(subs)]
    own_ids = id_row.astype(jnp.float32)

    def pick(first, id_rows):
        picks = jnp.concatenate([hot_of(row) for row in id_rows], axis=1).astype(jnp.bfloat16)
        lanes = slice(first * coefs, (first + len(id_rows)) * coefs)
        for r in range(0, order, 2 * LANES):
            chunk = slice(r, min(r + 2 * LANES, order))
            for i, half in enumerate(halves(global_ref[chunk])):
                picked_ref[i, chunk, lanes] = dot(half, picks, NN, None).astype(jnp.bfloat16)

    tables.wait_recv(range(2))
    arrived = [tables.arrived(1)[:coefs], tables.arrived(0)[:coefs]]
    for i in range(2):
        put(swapped_basis, (i,), arrived[i])
    id_rows = [own_ids] + [tables.slots[i][coefs : coefs + 1] for i in (1, 0)]
    pick(0, id_rows)
    for i in range(1, 3):
        put_corners(i, id_rows[i], arrived[i - 1])
    rhs_swap.wait_recv(range(2))
    tables.wait_recv(range(2, 4))
    from_prev, from_next = tables.arrived(2), tables.arrived(3)
    across = [
        (from_next if s % 2 else from_prev)[s // 2 * width : (s // 2 + 1) * width]
        for s in range(subs)
    ]
    across = jnp.concatenate(across, axis=0)
    put(swapped_basis, (2,), across)
    odd = lax.rem(lane // width, 2) == 1
    cross_ids = [tables.slots[i][coefs // 2 : coefs // 2 + 1] for i in (3, 2)]
    cross_ids = jnp.where(odd, *cross_ids)
    pick(3, [cross_ids])
    put_corners(3, cross_ids, across)
    across = across * jnp.concatenate(
        [
            jnp.broadcast_to(sign[loads * s : loads * s + 1, outer], (width, LANES))
            for s in partner
        ],
        axis=0,
    )
    rhs_swap.wait_recv(range(2, 4))
    rhs_swapped = rhs_swap.field()

    fix, fix_swapped, last, _ = correction(tail, share)
    fix_swapped = jnp.concatenate([fix_swapped, last()[0]], axis=1)
    direction = rhs - fix
    direction_swapped = rhs_swapped - fix_swapped
    spread = sign * (direction + direction_swapped)
    spread_bf = spread.astype(jnp.bfloat16)
    everything = slice(0, dual)
    image = image_of(spread_bf, everything, outer)
    rest = image_of(spread_bf, everything, inner)
    cross = swapped_raw(stacked(sign[:, outer] * image), 2, slice(0, LANES))
    image = jnp.concatenate([rest, image], axis=1)
    signed = sign * image
    halved = stacked(signed)
    corner_raw = raw_of(halved, everything, corner_rows, corner_lanes)
    raw = [own_raw(halved)]
    raw += [swapped_raw(halved, i, slice(i * LANES, (i + 1) * LANES)) for i in range(2)]
    cross_refs[0][...] = cross
    run(cross_copies, "start")
    tail, share, solve = sums(1, raw, corner_raw, corner_hot[...], dots(spread * image, rhs * rhs))
    tail.start()
    run(coarse_copies[:1], "wait_recv", has_high)
    run(coarse_copies[1:], "wait_recv", has_low)
    for slot, has in enumerate((has_high, has_low)):
        put_solve((slot + 1) * coefs, jnp.where(has, near_coarse[slot], 0.0))
    solve()
    share.start()
    for s in range(subs):
        mine = slice(partner[s] * width, (partner[s] + 1) * width)
        x = dot(stacked(across[mine])[0], ops_ref[s, outer, :], NN, None)
        put(cross_image, (mine,), x[:width] + x[width:])
    swap = Swap(swap_refs, 0)
    swap.fill(signed, orders, loads)
    swap.start()
    cross_wait(0, has_prev)
    cross_wait(1, has_next)
    from_prev = jnp.where(has_prev, cross_refs[1][0], 0.0)
    from_next = jnp.where(has_next, cross_refs[1][1], 0.0)
    share_out(2, jnp.where(odd, from_prev, from_next))
    late = Shares(2)
    late.start()
    swap.wait_recv()
    signed_swapped = swap.field()
    product = signed + signed_swapped
    product_swapped = signed_swapped + there * signed

    fix, fix_swapped, last, row = correction(tail, share, late)
    curvature, rho = as_column(row), as_column(row, loads)
    step = rho / curvature
    residual = rhs - step * product
    moved = direction - step * (product - fix)

    fix_swapped = jnp.concatenate([fix_swapped, jnp.zeros((rows, LANES), jnp.float32)], axis=1)
    moved_swapped = direction_swapped - step * (product_swapped - fix_swapped)
    spread_moved = sign * (moved + moved_swapped)
    image_moved = image_of(stacked(spread_moved)[0], everything, everything)
    residual_lanes = summed_lanes(residual * residual)
    last_fix, masked = last()
    image_moved = image_moved + step * dot3(masked, cross_image)
    last_fix = step * sign[:, outer] * last_fix
    spread_moved = jnp.concatenate(
        [spread_moved[:, inner], spread_moved[:, outer] + last_fix], axis=1
    )
    curve_refs[0][0] = dots(
        residual_lanes,
        spread_moved * image_moved,
        spread_moved * image + spread * image_moved,
    )
    curve = AllSum(sizes, curve_refs, 0)
    curve.start()
    signed = sign * image_moved
    last_swap = Swap(swap_refs, 1)
    last_swap.fill(signed, orders, loads)
    last_swap.start()
    last_swap.wait_recv()
    product_moved = signed + last_swap.field()
    for spread in open_sends + [swap]:
        spread.wait_send()
    each(members - 1, lambda k: gather_copy(k).wait_send())
    run(coarse_copies[:1], "wait_send", has_low)
    run(coarse_copies[1:], "wait_send", has_high)
    run(cross_copies, "wait_send")
    cross_wait(2, my_c == clusters - 2)
    cross_wait(3, my_c == 1)
    row = curve.finish()
    ratio = as_column(row) / rho
    last_curvature = as_column(row, loads) + ratio * (
        as_column(row, 2 * loads) + ratio * curvature
    )
    last_step = ratio * rho / last_curvature
    multipliers = (step + last_step * ratio) * direction + last_step * moved
    residual = residual - last_step * (product_moved + ratio * product)
    for s in range(subs):
        out_ref[0, s] = multipliers[s * loads : (s + 1) * loads]
        out_ref[1, s] = residual[s * loads : (s + 1) * loads]
    curve.wait_send()
    last_swap.wait_send()


def split(both_ref, mult_ref, res_ref, sems):
    copies = [
        pltpu.make_async_copy(both_ref.at[i], out, sems.at[i])
        for i, out in enumerate((mult_ref, res_ref))
    ]
    for copy in copies:
        copy.start()
    for copy in copies:
        copy.wait()


def local(sizes, *args):
    args = list(args)
    args[3] = jnp.transpose(args[3], (1, 0, 2))
    rhs, operators, signs, links, cluster_basis, corner_basis, ids, coarse, glob = args
    clusters, members = sizes
    subs, loads, dual = rhs.shape
    corn = corner_basis.shape[1]
    coefs = subs * (cluster_basis.shape[1] + corn)
    depth, order = glob.shape
    f32 = jnp.float32
    dma = pltpu.SemaphoreType.DMA

    def exchange(lead, block, receive):
        return [
            pltpu.VMEM(lead[:1] + block, f32),
            pltpu.VMEM(lead + receive, f32),
            dma(lead),
            dma(lead),
        ]

    def swap_scratch(count, height, extra):
        scratch = []
        for rows in (subs * height + extra, subs * height // 2 + extra):
            scratch += [
                pltpu.VMEM((count, 2, rows, LANES), f32),
                pltpu.VMEM((count, 2, rows, LANES), f32),
                dma((count, 2)),
                dma((count, 2)),
            ]
        return scratch

    def sum_scratch(count, block):
        scratch = []
        for axes in stages(sizes):
            scratch += exchange((count, peers_of(sizes, axes)), block, block)
        return scratch

    vmem = pl.BlockSpec(memory_space=pltpu.VMEM)
    scratch = [pltpu.VMEM(a.shape, a.dtype) for a in args]
    scratch[6] = pltpu.SMEM(ids.shape, ids.dtype)
    bf16 = jnp.bfloat16
    solved = members * coefs
    inside, columns = coarse.shape[1:]
    scratch += [
        dma((len(args),)),
        pltpu.VMEM((coefs, dual), f32),
        pltpu.VMEM((2, coefs, dual), bf16),
        pltpu.VMEM((2, 3, coefs, LANES), bf16),
        pltpu.VMEM((2, 3 * coefs, solved), bf16),
        pltpu.VMEM((coefs, order), bf16),
        pltpu.VMEM((2, 4 * subs * corn, dual), bf16),
        pltpu.VMEM((4 * subs * corn, order), bf16),
        pltpu.VMEM((order, order), f32),
        pltpu.VMEM((2, order, 4 * coefs), bf16),
        dma((members - 1,)),
        dma((members - 1,)),
        pltpu.VMEM((2, inside, columns), f32),
        dma((2,)),
        dma((2,)),
        pltpu.VMEM((loads, coefs), f32),
        pltpu.VMEM((4, loads, coefs), f32),
        dma((2,)),
        dma((4,)),
        pltpu.VMEM((2, coefs, dual), bf16),
        pltpu.VMEM((ITERS + 1, members, loads, coefs), f32),
    ]
    block, near = (loads, coefs), (min(3, members), loads, coefs)
    for lead, shape in (
        ((ITERS + 1, members), near),
        ((ITERS + 1, 2, members), block),
    ):
        scratch += [pltpu.VMEM(lead + shape, f32), dma(lead), dma(lead)]
    scratch += sum_scratch(1, (loads, order)) + sum_scratch(1, (loads + 1, order))
    scratch += sum_scratch(1, (1, LANES))
    scratch += swap_scratch(ITERS + 1, loads, 0)
    scratch += swap_scratch(1, coefs // subs, 8)
    both = pl.pallas_call(
        functools.partial(kernel, sizes),
        out_shape=pltpu.VMEM((2,) + rhs.shape, f32),
        in_specs=[pl.BlockSpec(memory_space=pltpu.HBM)] * len(args),
        out_specs=vmem,
        scratch_shapes=scratch,
        compiler_params=pltpu.CompilerParams(
            collective_id=0, has_side_effects=True, vmem_limit_bytes=56 << 20
        ),
    )(*args)
    return pl.pallas_call(
        split,
        out_shape=[jax.ShapeDtypeStruct(rhs.shape, f32)] * 2,
        in_specs=[vmem],
        out_specs=[pl.BlockSpec(memory_space=pltpu.HBM)] * 2,
        scratch_shapes=[dma((2,))],
        compiler_params=pltpu.CompilerParams(vmem_limit_bytes=4 << 20),
    )(both)


def solution(mesh):
    placed = (
        P(("cluster", "sub"), None, None),
        P(("cluster", "sub"), None, None),
        P(("cluster", "sub"), None),
        P(("cluster", "sub"), None, None),
        P(("cluster", "sub"), None, None),
        P(("cluster", "sub"), None, None),
        P(("cluster", "sub"), None),
        P("cluster", "sub", None),
        P("sub", None),
    )
    return jax.shard_map(
        functools.partial(local, (mesh.shape["cluster"], mesh.shape["sub"])),
        mesh=mesh,
        in_specs=placed,
        out_specs=(P(("cluster", "sub"), None, None), P(("cluster", "sub"), None, None)),
        check_vma=False,
    )
```
